32 devices in a mesh: replica: 8 (over z, x), shard: 4 (over y, core).
Axes of the slice: x: 2, y: 2, z: 4, core: 2. Of those that a mesh axis runs over, the one named last changes fastest.
Arguments:
- activations: bfloat16 [8192, 1536], P('replica'), may hold values from -6 to 6
- output_grads: bfloat16 [8192, 4, 1536], P('replica', None, 'shard'), may hold values from -0.009765625 to 0.009765625
- owner: int32 [4], replicated, may hold values from 0 to 3, each once
- step_count: int32 [1], replicated, may hold values from 1 to 40
- statistics: float32 [6144, 2, 1536], P(('replica', 'shard')), may hold values from -6 to 6
- inverse_roots: bfloat16 [6144, 2, 1536], P(('replica', 'shard')), may hold values from -1 to 2, as said below
- first_moment: float32 [6144, 1536], P(('replica', 'shard')), may hold values from -0.6 to 0.6
- second_moment: float32 [6144, 1536], P(('replica', 'shard')), may hold values from 0.005 to 0.05
Outputs:
- new_statistics: float32 [6144, 2, 1536], P(('replica', 'shard'))
- new_first: float32 [6144, 1536], P(('replica', 'shard'))
- new_second: float32 [6144, 1536], P(('replica', 'shard'))
- update: bfloat16 [4, 1536, 1536], P(None, None, 'shard')
The draws below stay inside these ranges and needn't reach their ends.
Inputs may be any that keep to these rules, and one draw needn't show every extreme that they name: A permutation: block b belongs to the group of replicas b' * (2) to (b' + 1) * 2 - 1 with b' = owner[b]. `inverse_roots`: each matrix has positive diagonal entries.
All inputs are finite; a program needn't handle non-finite values.
Results may differ from the reference program's by a relative error of at most 0.0049.
Values may be sent and summed in bfloat16 or wider, within the bound.
A program may use at most 128 MiB of HBM per device.

```python
import math
import jax
import jax.numpy as jnp
from jax import lax

D = 1536
BLOCKS = 4
TOKENS = 8192


def draw_inverse_roots(key, part):
    base_key = jax.random.fold_in(key, 11)
    key_noise, key_diagonal = jax.random.split(base_key, 2)
    scatter_noise = jax.random.normal(key_noise, (BLOCKS * D, 2, D), jnp.float32) * (0.5 / math.sqrt(D))
    diagonal = jax.random.uniform(key_diagonal, (BLOCKS * D, 2, 1), jnp.float32, 0.5, 1.5)
    within_rows = (jnp.arange(BLOCKS * D, dtype=jnp.int32) % D)[:, None, None]
    column_ids = jnp.arange(D, dtype=jnp.int32)[None, None, :]
    return (scatter_noise + jnp.where(within_rows == column_ids, diagonal, 0.0)).astype(jnp.bfloat16)


def steps_of(stream_key, extent, cuts, low, largest):
    def one(position, shards_of):
        heights = jax.random.uniform(jax.random.fold_in(jax.random.fold_in(stream_key, 6), position), (shards_of,), jnp.float32, low / len(cuts), largest / len(cuts))
        return jnp.repeat(jnp.exp(heights), extent[position] // shards_of).reshape((-1,) + (1,) * (len(extent) - position - 1))

    loudness = one(*cuts[0])
    for cut in cuts[1:]:
        loudness = loudness * one(*cut)
    return loudness


def centred(own_key, dims, deviation, limit, shards=(), kind=jnp.bfloat16):
    values = jax.random.normal(own_key, dims, jnp.float32) * deviation
    if len(shards) > 0:
        values = steps_of(own_key, dims, shards, -0.22, 0.18) * values
    return jnp.clip(values, min=-limit, max=limit).astype(kind)


def setup_inputs(seed: int = 0) -> dict:
    splits = jax.random.split(jax.random.key(seed), 9)
    return {
        "activations": centred(splits[0], (TOKENS, D), 1.0, 6.0, ((0, 8),)),
        "output_grads": centred(splits[1], (TOKENS, BLOCKS, D), (TOKENS * 40) ** -0.5, 0.009765625, ((0, 8), (2, 4))),
        "owner": jax.random.permutation(splits[2], BLOCKS).astype(jnp.int32),
        "step_count": jax.random.randint(splits[3], (1,), 1, 41).astype(jnp.int32),
        "statistics": centred(splits[4], (BLOCKS * D, 2, D), 1.0, 6.0, ((0, 32),), jnp.float32),
        "inverse_roots": draw_inverse_roots(jax.random.fold_in(splits[8], 71), 0),
        "first_moment": centred(splits[6], (BLOCKS * D, D), 0.1, 0.6, ((0, 32),), jnp.float32),
        "second_moment": jnp.clip(jnp.exp(math.log(0.05) - 2.3025851 * jax.random.uniform(splits[7], (BLOCKS * D, D), jnp.float32) ** steps_of(splits[7], (BLOCKS * D, D), ((0, 32),), -0.2, 0.2)), 0.005, 0.05),
    }


beta_stat = 0.9
beta_first = 0.9
beta_second = 0.999
eps_adam = 1e-08
eps_norm = 1e-06

def reference(activations, output_grads, owner, step_count, statistics, inverse_roots, first_moment, second_moment):
    blocks_count = output_grads.shape[1]
    model_width = activations.shape[1]
    slot_ids = jnp.arange(blocks_count, dtype=jnp.int32)
    onehot = (owner[None, :] == slot_ids[:, None]).astype(jnp.int32)
    source = lax.optimization_barrier(jnp.sum(onehot * slot_ids[None, :], axis=1)).astype(jnp.int32)

    def block_grad(block_index):
        douts = lax.dynamic_index_in_dim(output_grads, block_index, 1, keepdims=False)
        return lax.dot_general(activations, douts, (((0,), (0,)), ((), ())), preferred_element_type=jnp.float32)
    exact = lax.map(block_grad, source)
    rounded = exact.astype(jnp.bfloat16)
    stats_slot = statistics.reshape(blocks_count, model_width, 2, model_width)
    roots_slot = inverse_roots.reshape(blocks_count, model_width, 2, model_width)

    def precondition(operands):
        grad_block, stat_block, root_block = operands
        left_gram = lax.dot_general(grad_block, grad_block, (((1,), (1,)), ((), ())), preferred_element_type=jnp.float32)
        right_gram = lax.dot_general(grad_block, grad_block, (((0,), (0,)), ((), ())), preferred_element_type=jnp.float32)
        new_left = beta_stat * stat_block[:, 0, :] + (1.0 - beta_stat) * left_gram
        new_right = beta_stat * stat_block[:, 1, :] + (1.0 - beta_stat) * right_gram
        right_part = lax.dot_general(grad_block, root_block[:, 1, :], (((1,), (1,)), ((), ())), preferred_element_type=jnp.float32)
        precond = jnp.dot(root_block[:, 0, :].astype(jnp.float32), right_part, precision=lax.Precision.HIGHEST)
        return (jnp.stack([new_left, new_right], axis=1), precond)
    new_stats, precond = lax.map(precondition, (rounded, stats_slot, roots_slot))
    flat_grad = exact.reshape(blocks_count * model_width, model_width)
    count_float = step_count[0].astype(jnp.float32)
    first_new = beta_first * first_moment + (1.0 - beta_first) * flat_grad
    second_new = beta_second * second_moment + (1.0 - beta_second) * flat_grad * flat_grad
    first_hat = first_new / (1.0 - jnp.power(beta_first, count_float))
    second_hat = second_new / (1.0 - jnp.power(beta_second, count_float))
    adam_dir = first_hat / (jnp.sqrt(second_hat) + eps_adam)
    adam_squares = lax.optimization_barrier(jnp.sum((adam_dir * adam_dir).reshape(blocks_count, -1), axis=1))
    precond_squares = lax.optimization_barrier(jnp.sum((precond * precond).reshape(blocks_count, -1), axis=1))
    scale = jnp.sqrt(adam_squares) / (jnp.sqrt(precond_squares) + eps_norm)
    grafted = (precond * scale[:, None, None]).astype(jnp.bfloat16)
    update = jnp.take(grafted, owner, axis=0)
    return (new_stats.reshape(blocks_count * model_width, 2, model_width), first_new, second_new, update)
```

```python
import functools

import jax
import jax.numpy as jnp
import numpy as np
from jax import lax
from jax.experimental import pallas as pl
from jax.experimental.pallas import tpu as pltpu
from jax.sharding import PartitionSpec as P

beta_stat = 0.9
beta_first = 0.9
beta_second = 0.999
eps_adam = 1e-08
eps_norm = 1e-06


def bits_of(extent):
    return extent.bit_length() - 1


def swap(value, axis, bit, keep=lambda i: True):
    n = lax.axis_size(axis)
    return lax.ppermute(value, axis, [(i, i ^ (1 << bit)) for i in range(n) if keep(i)])


def join(value, partner, axis, bit, dim):
    upper = (lax.axis_index(axis) >> bit) & 1 == 1
    return jnp.where(
        upper,
        jnp.concatenate([partner, value], dim),
        jnp.concatenate([value, partner], dim),
    )


def double(value, axis, bit, dim, keep=lambda i: True):
    return join(value, swap(value, axis, bit, keep), axis, bit, dim)


def reversed_bits(count):
    bits = bits_of(count)
    return [int(format(i, "b").zfill(bits)[::-1], 2) if bits else 0 for i in range(count)]


def reorder(value, count, dim):
    size = value.shape[dim] // count
    return jnp.concatenate(
        [lax.slice_in_dim(value, k * size, (k + 1) * size, axis=dim) for k in reversed_bits(count)],
        dim,
    )


def choose(values, picks, slot):
    out = values[picks[max(picks)]]
    for z in sorted(picks):
        if values[picks[z]] is not out:
            out = jnp.where(slot == z, values[picks[z]], out)
    return out


def body(
    activations,
    output_grads,
    owner,
    step_count,
    statistics,
    inverse_roots,
    first_moment,
    second_moment,
):
    f32, bf16 = jnp.float32, jnp.bfloat16
    width = activations.shape[1]
    groups = output_grads.shape[1]
    replicas = lax.axis_size("replica")
    shards = lax.axis_size("shard")
    size = replicas // groups
    local_bits = range(bits_of(size))
    shard_bits = list(range(bits_of(shards)))[::-1]
    span = statistics.shape[0]
    replica = lax.axis_index("replica")
    slot, local = replica // size, replica % size
    shard = lax.axis_index("shard")
    span_index = local * shards + shard

    slot_ids = jnp.arange(groups, dtype=jnp.int32)
    onehot = (owner[None, :] == slot_ids[:, None]).astype(jnp.int32)
    source = jnp.sum(onehot * slot_ids[None, :], axis=1)

    order = [sorted(range(groups), key=lambda s: (-abs(s - z), s)) for z in range(groups)]
    block_order = jnp.take(source, jnp.take(jnp.asarray(np.array(order, np.int32)), slot, axis=0))
    douts = output_grads.transpose(1, 0, 2)
    rounds = []
    for k in range(groups):
        part = lax.dot_general(
            activations,
            lax.dynamic_index_in_dim(douts, block_order[k], 0, keepdims=False),
            (((0,), (0,)), ((), ())),
            preferred_element_type=f32,
        )
        for bit in list(local_bits)[::-1]:
            half = part.shape[0] // 2
            mine = (local >> bit) & 1
            away = lax.dynamic_slice_in_dim(part, (1 - mine) * half, half, 0).astype(bf16)
            part = lax.dynamic_slice_in_dim(part, mine * half, half, 0) + swap(
                away, "replica", bit
            ).astype(f32)
        rounds.append(part)

    def shift(value, up, senders):
        step = size if up else -size
        return lax.ppermute(
            value,
            "replica",
            [(r, r + step) for r in range(replicas) if r // size in senders],
        )

    came_up = came_down = None
    for t in range(1, groups):
        ups = {z: order[z].index(groups - t + z) for z in range(t)}
        downs = {z: order[z].index(z + t - groups) for z in range(groups - t, groups)}
        up = choose(rounds, ups, slot)
        down = choose(rounds, downs, slot)
        if came_up is not None:
            up = up + came_up.astype(f32)
            down = down + came_down.astype(f32)
        came_up = shift(up.astype(bf16), True, ups)
        came_down = shift(down.astype(bf16), False, downs)
    own = (rounds[-1] + came_up.astype(f32) + came_down.astype(f32)).astype(bf16)

    rows = own.shape[0]
    top, low = own[: rows // 2], own[rows // 2 :]
    for bit in local_bits:
        top = double(top, "replica", bit, 0)
    for bit in shard_bits[:-1]:
        low = double(low, "shard", bit, 1)
        top = double(top, "shard", bit, 1)
    for bit in local_bits:
        low = double(low, "replica", bit, 0)
    for bit in shard_bits[-1:]:
        low = double(low, "shard", bit, 1)
        top = double(top, "shard", bit, 1)
    pieces = []
    for k in range(size):
        for half in (top, low):
            pieces.append(lax.slice_in_dim(half, k * (rows // 2), (k + 1) * (rows // 2), axis=0))
    full_grad = reorder(jnp.concatenate(pieces, 0), shards, 1)

    left_root = inverse_roots[:, 0, :]
    for bit in shard_bits:
        left_root = double(left_root, "shard", bit, 0)
    left_root = reorder(left_root, shards, 0)
    pairs = []
    for r in range(replicas):
        for s in range(shards):
            j = (r % size) * shards + s
            target = (r // size * size + j % size) * shards + j // size
            pairs.append((r * shards + s, target))
    right_root = lax.ppermute(inverse_roots[:, 1, :], ("replica", "shard"), pairs)
    for bit in local_bits:
        right_root = double(right_root, "replica", bit, 0)

    right_part = lax.dot_general(
        full_grad, right_root, (((1,), (1,)), ((), ())), preferred_element_type=f32
    )
    high = lax.reduce_precision(right_part, 8, 7)
    rest = right_part - high
    precond = jnp.dot(left_root, high.astype(bf16), preferred_element_type=f32) + jnp.dot(
        left_root, rest.astype(bf16), preferred_element_type=f32
    )

    rounded = lax.dynamic_slice_in_dim(full_grad, span_index * span, span, 0)
    exact = rounded.astype(f32)
    count_float = step_count[0].astype(f32)
    first_new = beta_first * first_moment + (1.0 - beta_first) * exact
    second_new = beta_second * second_moment + (1.0 - beta_second) * exact * exact
    first_hat = first_new / (1.0 - jnp.power(beta_first, count_float))
    second_hat = second_new / (1.0 - jnp.power(beta_second, count_float))
    adam_dir = first_hat / (jnp.sqrt(second_hat) + eps_adam)

    sums = jnp.stack([jnp.sum(adam_dir * adam_dir), jnp.sum(precond * precond)])
    sums = jnp.broadcast_to(sums[:, None], (2, 128))
    for bit in local_bits:
        sums = sums + swap(sums, "replica", bit)
    for bit in shard_bits:
        sums = sums + swap(sums, "shard", bit)
    scale = jnp.sqrt(sums[0, 0]) / (jnp.sqrt(sums[1, 0]) + eps_norm)
    grafted = (precond * scale).astype(bf16)

    def complete(value, zs):
        for bit in local_bits:
            value = double(value, "replica", bit, 0, lambda r: r // size in zs)
        return value

    whole = {0: complete(grafted, range(groups))}
    up = down = grafted
    ups, downs = {}, {}
    for t in range(1, groups):
        up = shift(up, True, range(t - 1, groups - 1))
        down = shift(down, False, range(1, groups - t + 1))
        ups[t] = complete(up, range(t, groups))
        downs[t] = complete(down, range(0, groups - t))
    for m in range(1, groups):
        whole[m] = jnp.where(slot + m < groups, downs[m], ups[groups - m])
    update = jnp.zeros((groups,) + whole[0].shape, bf16)
    for m in range(groups):
        block = jnp.take(source, (slot + m) % groups)
        update = lax.dynamic_update_index_in_dim(update, whole[m], block, 0)

    grad_columns = lax.dynamic_slice_in_dim(full_grad, span_index * span, span, 1)
    left_gram = lax.dot_general(
        rounded, full_grad, (((1,), (1,)), ((), ())), preferred_element_type=f32
    )
    right_gram = lax.dot_general(
        grad_columns, full_grad, (((0,), (0,)), ((), ())), preferred_element_type=f32
    )
    new_left = beta_stat * statistics[:, 0, :] + (1.0 - beta_stat) * left_gram
    new_right = beta_stat * statistics[:, 1, :] + (1.0 - beta_stat) * right_gram
    new_stats = jnp.stack([new_left, new_right], axis=1)
    return (new_stats, first_new, second_new, update)


PARTS = 2


def is_equal(a, b):
    return lax.div(jnp.int32(1), 1 + (a - b) * (a - b))


def block_orders(groups):
    return [sorted(range(groups), key=lambda s: (-abs(s - z), s)) for z in range(groups)]


def step_kernel(
    groups,
    source_ref,
    bias_ref,
    at_hbm,
    d_hbm,
    left_hbm,
    right_hbm,
    first_hbm,
    second_hbm,
    update_hbm,
    first_out,
    second_out,
    left_out,
    right_out,
    at,
    d,
    acc,
    x_send,
    x_recv,
    z_send,
    up_recv,
    down_recv,
    g,
    left,
    right,
    stage,
    high,
    low,
    precond,
    first,
    second,
    columns,
    left_gram,
    right_gram,
    u,
    norms,
    load_sem,
    out_sem,
    u_out_sem,
    x_ssem,
    x_rsem,
    z_ssem,
    up_rsem,
    down_rsem,
    g_ssem,
    g_rsem,
    l_ssem,
    l_rsem,
    r_ssem,
    r_rsem,
    n_ssem,
    n_rsem,
    ux_ssem,
    ux_rsem,
    uz_ssem,
    uu_rsem,
    ud_rsem,
):
    f32, bf16 = jnp.float32, jnp.bfloat16
    Z, Q = groups, PARTS
    width = g.shape[0]
    half = width // 2
    rows = half // Q
    cols = d.shape[2]
    span = first.shape[0]
    replica, s = lax.axis_index("replica"), lax.axis_index("shard")
    z, x = lax.div(replica, 2), lax.rem(replica, 2)
    y, c = lax.div(s, 2), lax.rem(s, 2)
    i = x * 4 + s
    x_dev = (z * 2 + 1 - x, s)
    y_dev = (replica, (1 - y) * 2 + c)
    c_dev = (replica, y * 2 + 1 - c)
    up_dev = (replica + 2, s)
    down_dev = (replica - 2, s)

    def remote(src, dst, ssem, rsem, dev):
        return pltpu.make_async_remote_copy(
            src_ref=src,
            dst_ref=dst,
            send_sem=ssem,
            recv_sem=rsem,
            device_id=dev,
            device_id_type=pl.DeviceIdType.MESH,
        )

    def peer(k):
        j = lax.rem(i + k, 8)
        return (z * 2 + lax.div(j, 4), lax.rem(j, 4))

    def left_rows(shard):
        return left.at[pl.ds(pl.multiple_of(shard * span, span), span)]

    loads = [
        pltpu.make_async_copy(at_hbm, at, load_sem.at[0]),
        pltpu.make_async_copy(d_hbm, d, load_sem.at[1]),
        pltpu.make_async_copy(left_hbm, left_rows(s), load_sem.at[2]),
        pltpu.make_async_copy(right_hbm, stage, load_sem.at[3]),
        pltpu.make_async_copy(first_hbm, first, load_sem.at[4]),
        pltpu.make_async_copy(second_hbm, second, load_sem.at[5]),
    ]
    for load in loads:
        load.start()

    barrier = pltpu.get_barrier_semaphore()

    def greet(dev):
        pl.semaphore_signal(barrier, inc=1, device_id=dev, device_id_type=pl.DeviceIdType.MESH)

    for k in range(1, 8):
        greet(peer(k))
    has_below, has_above = z > 0, z < Z - 1

    @pl.when(has_above)
    def _():
        greet(up_dev)

    @pl.when(has_below)
    def _():
        greet(down_dev)

    pl.semaphore_wait(barrier, 9 - is_equal(z, 0) - is_equal(z, Z - 1))

    loads[2].wait()
    l_y = remote(left_rows(s), left_rows(s), l_ssem.at[0], l_rsem.at[0], y_dev)
    l_c = remote(left_rows(s), left_rows(s), l_ssem.at[1], l_rsem.at[1], c_dev)
    s_y, s_c = (1 - y) * 2 + c, y * 2 + 1 - c
    l_f = remote(left_rows(s_y), left_rows(s_y), l_ssem.at[2], l_rsem.at[2], c_dev)
    l_y.start()
    l_c.start()
    loads[0].wait()
    loads[1].wait()

    orders = block_orders(Z)

    def target(k):
        return sum(
            is_equal(z, a) * is_equal(k, b) * orders[a][b] for a in range(Z) for b in range(Z)
        )

    def x_copy(k, q):
        return remote(x_send.at[k, q], x_recv.at[k, q], x_ssem.at[k, q], x_rsem.at[k, q], x_dev)

    def multiply(n, carry):
        k, q = lax.div(n, Q), lax.rem(n, Q)
        block = source_ref[target(k)]
        away = pl.multiple_of((1 - x) * half + q * rows, rows)
        mine = pl.multiple_of(x * half + q * rows, rows)
        x_send[k, q] = jnp.dot(
            at[pl.ds(away, rows), :], d[block], preferred_element_type=f32
        ).astype(bf16)
        x_copy(k, q).start()
        acc[k, q] = jnp.dot(at[pl.ds(mine, rows), :], d[block], preferred_element_type=f32)
        return carry

    lax.fori_loop(0, Z * Q, multiply, 0)

    loads[3].wait()
    place = right.at[pl.ds(pl.multiple_of(c * span, span), span)]
    at_home = is_equal(x, y) * is_equal(y, c)

    def r_copy(tx):
        return remote(stage, place, r_ssem.at[tx], r_rsem.at[c], (z * 2 + tx, x * 2 + y))

    r_local = pltpu.make_async_copy(right_hbm, place, load_sem.at[6])
    for tx in range(2):

        @pl.when(is_equal(x, tx) * at_home == 0)
        def _(tx=tx):
            r_copy(tx).start()

    @pl.when(at_home == 1)
    def _():
        r_local.start()

    l_y.wait_recv()
    l_f.start()

    def up_copy(k, q, t):
        return remote(z_send.at[k, q], up_recv.at[t, q], z_ssem.at[k, q], up_rsem.at[t, q], up_dev)

    def down_copy(k, q, t):
        return remote(
            z_send.at[k, q], down_recv.at[t, q], z_ssem.at[k, q], down_rsem.at[t, q], down_dev
        )

    def gather(k, q, t, from_below, from_above):
        x_copy(k, q).wait_recv()
        acc[k, q] = acc[k, q] + x_recv[k, q].astype(f32)

        @pl.when(from_below)
        def _():
            up_copy(k, q, t).wait_recv()
            acc[k, q] = acc[k, q] + up_recv[t, q].astype(f32)

        @pl.when(from_above)
        def _():
            down_copy(k, q, t).wait_recv()
            acc[k, q] = acc[k, q] + down_recv[t, q].astype(f32)

    def pass_on(n, carry):
        k, q = lax.div(n, Q), lax.rem(n, Q)
        t = target(k)
        gather(k, q, t, (t > z) & has_below, (t < z) & has_above)
        z_send[k, q] = acc[k, q].astype(bf16)

        @pl.when(t > z)
        def _():
            up_copy(k, q, t).start()

        @pl.when(t < z)
        def _():
            down_copy(k, q, t).start()

        return carry

    lax.fori_loop(0, (Z - 1) * Q, pass_on, 0)

    def tile(xt, yt, ct, q):
        top = pl.multiple_of(xt * half + q * rows, rows)
        side = pl.multiple_of((yt * 2 + ct) * cols, cols)
        return g.at[pl.ds(top, rows), pl.ds(side, cols)]

    def g_copy(rel, q):
        xt, yt, ct, dev = (
            (x, y, c, c_dev),
            (x, y, c, y_dev),
            (x, y, c, x_dev),
            (1 - x, y, c, y_dev),
            (x, 1 - y, c, c_dev),
            (1 - x, y, c, c_dev),
            (1 - x, 1 - y, c, c_dev),
        )[rel]
        ref = tile(xt, yt, ct, q)
        return remote(ref, ref, g_ssem.at[rel, q], g_rsem.at[rel, q], dev)

    for q in range(Q):
        gather(Z - 1, q, z, has_below, has_above)
        tile(x, y, c, q)[...] = acc[Z - 1, q].astype(bf16)
        for rel in (2, 1, 0):
            g_copy(rel, q).start()
    for q in range(Q):
        g_copy(2, q).wait_recv()
        g_copy(3, q).start()
        g_copy(5, q).start()
        g_copy(1, q).wait_recv()
        g_copy(4, q).start()
    for q in range(Q):
        g_copy(3, q).wait_recv()
        g_copy(6, q).start()
    for q in range(Q):
        for rel in (0, 4, 5, 6):
            g_copy(rel, q).wait_recv()

    for rc in range(2):

        @pl.when(at_home * is_equal(c, rc) == 0)
        def _(rc=rc):
            remote(stage, right.at[pl.ds(rc * span, span)], r_ssem.at[0], r_rsem.at[rc], x_dev).wait_recv()

    @pl.when(at_home == 1)
    def _():
        r_local.wait()

    l_c.wait_recv()
    l_f.wait_recv()
    step = cols // 3 * 2 if cols % 3 == 0 else cols

    def times_right(n, carry):
        r = pl.ds(pl.multiple_of(n * step, step), step)
        value = lax.dot_general(
            g[r, :], right[...], (((1,), (1,)), ((), ())), preferred_element_type=f32
        )
        top = value.astype(bf16)
        high[r, :] = top
        low[r, :] = (value - top.astype(f32)).astype(bf16)
        return carry

    lax.fori_loop(0, width // step, times_right, 0)

    def times_left(n, total):
        r = pl.ds(pl.multiple_of(n * step, step), step)
        value = jnp.dot(left[r, :], high[...], preferred_element_type=f32) + jnp.dot(
            left[r, :], low[...], preferred_element_type=f32
        )
        precond[r, :] = value
        return total + jnp.sum(value * value)

    precond_squares = lax.fori_loop(0, half // step, times_left, jnp.float32(0))

    loads[4].wait()
    loads[5].wait()
    base = pl.multiple_of(i * span, span)
    lot = 16

    def adam(n, total):
        r = pl.ds(pl.multiple_of(n * lot, lot), lot)
        grad = g[pl.ds(pl.multiple_of(base + n * lot, lot), lot), :].astype(f32)
        first_new = beta_first * first[r, :] + (1.0 - beta_first) * grad
        second_new = beta_second * second[r, :] + (1.0 - beta_second) * grad * grad
        first[r, :] = first_new
        second[r, :] = second_new
        value = (first_new / bias_ref[0]) / (jnp.sqrt(second_new / bias_ref[1]) + eps_adam)
        return total + value * value

    adam_squares = jnp.sum(
        lax.fori_loop(0, span // lot, adam, jnp.zeros((lot, width), f32))
    )

    which = lax.broadcasted_iota(jnp.int32, norms.shape[1:], 0)
    norms[i] = jnp.where(which == 0, adam_squares, precond_squares)

    def n_copy(k):
        return remote(norms.at[i], norms.at[i], n_ssem.at[k - 1], n_rsem.at[i], peer(k))

    for k in range(1, 8):
        n_copy(k).start()
    outs = [
        pltpu.make_async_copy(first, first_out, out_sem.at[0]),
        pltpu.make_async_copy(second, second_out, out_sem.at[1]),
        pltpu.make_async_copy(left_gram, left_out, out_sem.at[2]),
        pltpu.make_async_copy(right_gram, right_out, out_sem.at[3]),
    ]
    outs[0].start()
    outs[1].start()
    for k in range(1, 8):
        j = lax.rem(i + k, 8)
        remote(norms.at[j], norms.at[j], n_ssem.at[k - 1], n_rsem.at[j], peer(k)).wait_recv()
    total = norms[0]
    for k in range(1, 8):
        total = total + norms[k]
    scale = jnp.sqrt(total[0:1, :]) / (jnp.sqrt(total[1:2, :]) + eps_norm)

    def part(zt, xt, q):
        top = pl.multiple_of(xt * half + q * rows, rows)
        return u.at[zt, pl.ds(top, rows), :]

    def ux_copy(zt, q):
        return remote(part(zt, x, q), part(zt, x, q), ux_ssem.at[zt, q], ux_rsem.at[zt, q], x_dev)

    def uu_copy(zt, q):
        return remote(part(zt, x, q), part(zt, x, q), uz_ssem.at[0, zt, q], uu_rsem.at[zt, q], up_dev)

    def ud_copy(zt, q):
        return remote(part(zt, x, q), part(zt, x, q), uz_ssem.at[1, zt, q], ud_rsem.at[zt, q], down_dev)

    def store(zt, xt, q):
        top = pl.multiple_of(xt * half + q * rows, rows)
        return pltpu.make_async_copy(
            part(zt, xt, q), update_hbm.at[zt, pl.ds(top, rows), :], u_out_sem.at[zt, xt, q]
        )

    for q in range(Q):
        part(z, x, q)[...] = (precond[pl.ds(q * rows, rows), :] * scale).astype(bf16)
        ux_copy(z, q).start()

        @pl.when(has_above)
        def _(q=q):
            uu_copy(z, q).start()

        @pl.when(has_below)
        def _(q=q):
            ud_copy(z, q).start()

        store(z, x, q).start()

    window = pl.multiple_of(lax.div(i, 2) * cols, cols)
    turned = g[:, pl.ds(window, cols)].T
    columns[...] = jnp.where(lax.rem(i, 2) == 1, turned[span:, :], turned[:span, :])

    def grams(n, carry):
        r = pl.ds(pl.multiple_of(n * cols, cols), cols)
        left_gram[:, r] = lax.dot_general(
            g[pl.ds(base, span), :], g[r, :], (((1,), (1,)), ((), ())), preferred_element_type=f32
        )
        right_gram[:, r] = jnp.dot(columns[...], g[:, r], preferred_element_type=f32)
        return carry

    lax.fori_loop(0, width // cols, grams, 0)
    outs[2].start()
    outs[3].start()

    for dist in range(1, Z):
        for q in range(Q):

            @pl.when(z - dist >= 0)
            def _(dist=dist, q=q):
                zt = z - dist
                uu_copy(zt, q).wait_recv()

                @pl.when(has_above)
                def _():
                    uu_copy(zt, q).start()

                ux_copy(zt, q).start()
                store(zt, x, q).start()

            @pl.when(z + dist < Z)
            def _(dist=dist, q=q):
                zt = z + dist
                ud_copy(zt, q).wait_recv()

                @pl.when(has_below)
                def _():
                    ud_copy(zt, q).start()

                ux_copy(zt, q).start()
                store(zt, x, q).start()

    def arrive(zt):
        for q in range(Q):
            ux_copy(zt, q).wait_recv()
            store(zt, 1 - x, q).start()

    arrive(z)
    for dist in range(1, Z):

        @pl.when(z - dist >= 0)
        def _(dist=dist):
            arrive(z - dist)

        @pl.when(z + dist < Z)
        def _(dist=dist):
            arrive(z + dist)

    l_y.wait_send()
    l_c.wait_send()
    l_f.wait_send()
    for tx in range(2):

        @pl.when(is_equal(x, tx) * at_home == 0)
        def _(tx=tx):
            r_copy(tx).wait_send()

    for k in range(1, 8):
        n_copy(k).wait_send()
    for k in range(Z):
        for q in range(Q):
            x_copy(k, q).wait_send()
            ux_copy(k, q).wait_send()
            store(k, 0, q).wait()
            store(k, 1, q).wait()
            if k < Z - 1:
                up_copy(k, q, k).wait_send()

            @pl.when((z >= k) & has_above)
            def _(k=k, q=q):
                uu_copy(k, q).wait_send()

            @pl.when((z <= k) & has_below)
            def _(k=k, q=q):
                ud_copy(k, q).wait_send()

    for rel in range(7):
        for q in range(Q):
            g_copy(rel, q).wait_send()
    for out in outs:
        out.wait()


def place_kernel(owner_ref, from_ref, to_ref):
    to_ref[...] = from_ref[...]


def fused_body(
    activations,
    output_grads,
    owner,
    step_count,
    statistics,
    inverse_roots,
    first_moment,
    second_moment,
):
    f32, bf16 = jnp.float32, jnp.bfloat16
    tokens, width = activations.shape
    groups, cols = output_grads.shape[1:]
    span = statistics.shape[0]
    half, Q = width // 2, PARTS
    rows = half // Q
    slot_ids = jnp.arange(groups, dtype=jnp.int32)
    onehot = (owner[None, :] == slot_ids[:, None]).astype(jnp.int32)
    source = jnp.sum(onehot * slot_ids[None, :], axis=1)
    count = step_count[0].astype(f32)
    bias = jnp.stack([1.0 - jnp.power(beta_first, count), 1.0 - jnp.power(beta_second, count)])

    VMEM, DMA = pltpu.VMEM, pltpu.SemaphoreType.DMA
    tiles = (groups, Q, rows, cols)
    hbm = pl.BlockSpec(memory_space=pl.ANY)
    smem = pl.BlockSpec(memory_space=pltpu.SMEM)
    grams = jax.ShapeDtypeStruct((span, width), f32)
    update, first_new, second_new, left_gram, right_gram = pl.pallas_call(
        functools.partial(step_kernel, groups),
        out_shape=(jax.ShapeDtypeStruct((groups, width, cols), bf16), grams, grams, grams, grams),
        in_specs=[smem, smem] + [hbm] * 6,
        out_specs=[hbm] * 5,
        scratch_shapes=[
            VMEM((width, tokens), bf16),
            VMEM((groups, tokens, cols), bf16),
            VMEM(tiles, f32),
            VMEM(tiles, bf16),
            VMEM(tiles, bf16),
            VMEM(tiles, bf16),
            VMEM(tiles, bf16),
            VMEM(tiles, bf16),
            VMEM((width, width), bf16),
            VMEM((half, width), bf16),
            VMEM((2 * span, width), bf16),
            VMEM((span, width), bf16),
            VMEM((width, cols), bf16),
            VMEM((width, cols), bf16),
            VMEM((half, cols), f32),
            VMEM((span, width), f32),
            VMEM((span, width), f32),
            VMEM((span, width), bf16),
            VMEM((span, width), f32),
            VMEM((span, width), f32),
            VMEM((groups, width, cols), bf16),
            VMEM((8, 8, cols), f32),
            DMA((7,)),
            DMA((4,)),
            DMA((groups, 2, Q)),
            DMA((groups, Q)),
            DMA((groups, Q)),
            DMA((groups, Q)),
            DMA((groups, Q)),
            DMA((groups, Q)),
            DMA((7, Q)),
            DMA((7, Q)),
            DMA((3,)),
            DMA((3,)),
            DMA((2,)),
            DMA((2,)),
            DMA((7,)),
            DMA((8,)),
            DMA((groups, Q)),
            DMA((groups, Q)),
            DMA((2, groups, Q)),
            DMA((groups, Q)),
            DMA((groups, Q)),
        ],
        compiler_params=pltpu.CompilerParams(
            collective_id=0, has_side_effects=True, vmem_limit_bytes=60 * 1024 * 1024
        ),
        name="step_kernel",
    )(
        source,
        bias,
        activations.T,
        output_grads.transpose(1, 0, 2),
        inverse_roots[:, 0, :],
        inverse_roots[:, 1, :],
        first_moment,
        second_moment,
    )

    placed = pl.pallas_call(
        place_kernel,
        out_shape=jax.ShapeDtypeStruct((groups, width, cols), bf16),
        grid_spec=pltpu.PrefetchScalarGridSpec(
            num_scalar_prefetch=1,
            grid=(groups, 2),
            in_specs=[pl.BlockSpec((1, half, cols), lambda b, h, o: (o[b], h, 0))],
            out_specs=pl.BlockSpec((1, half, cols), lambda b, h, o: (b, h, 0)),
        ),
        name="place_kernel",
    )(owner, update)
    grams = jnp.stack([left_gram, right_gram], axis=1)
    return (beta_stat * statistics + (1.0 - beta_stat) * grams, first_new, second_new, placed)


def dispatch(replicas, shards, *args):
    groups = args[1].shape[1]
    if replicas == 2 * groups and shards == 4:
        return fused_body(*args)
    return body(*args)


def solution(mesh):
    placed = (
        P("replica", None),
        P("replica", None, "shard"),
        P(),
        P(),
        P(("replica", "shard"), None, None),
        P(("replica", "shard"), None, None),
        P(("replica", "shard"), None),
        P(("replica", "shard"), None),
    )
    return jax.shard_map(
        functools.partial(dispatch, mesh.shape["replica"], mesh.shape["shard"]),
        mesh=mesh,
        in_specs=placed,
        out_specs=(
            P(("replica", "shard"), None, None),
            P(("replica", "shard"), None),
            P(("replica", "shard"), None),
            P(None, None, "shard"),
        ),
        check_vma=False,
    )
```

```python
import functools

import jax
import jax.numpy as jnp
import numpy as np
from jax import lax
from jax.experimental import pallas as pl
from jax.experimental.pallas import tpu as pltpu
from jax.sharding import PartitionSpec as P

beta_stat = 0.9
beta_first = 0.9
beta_second = 0.999
eps_adam = 1e-08
eps_norm = 1e-06


def bits_of(extent):
    return extent.bit_length() - 1


def swap(value, axis, bit, keep=lambda i: True):
    n = lax.axis_size(axis)
    return lax.ppermute(value, axis, [(i, i ^ (1 << bit)) for i in range(n) if keep(i)])


def join(value, partner, axis, bit, dim):
    upper = (lax.axis_index(axis) >> bit) & 1 == 1
    return jnp.where(
        upper,
        jnp.concatenate([partner, value], dim),
        jnp.concatenate([value, partner], dim),
    )


def double(value, axis, bit, dim, keep=lambda i: True):
    return join(value, swap(value, axis, bit, keep), axis, bit, dim)


def reversed_bits(count):
    bits = bits_of(count)
    return [int(format(i, "b").zfill(bits)[::-1], 2) if bits else 0 for i in range(count)]


def reorder(value, count, dim):
    size = value.shape[dim] // count
    return jnp.concatenate(
        [lax.slice_in_dim(value, k * size, (k + 1) * size, axis=dim) for k in reversed_bits(count)],
        dim,
    )


def choose(values, picks, slot):
    out = values[picks[max(picks)]]
    for z in sorted(picks):
        if values[picks[z]] is not out:
            out = jnp.where(slot == z, values[picks[z]], out)
    return out


def body(
    activations,
    output_grads,
    owner,
    step_count,
    statistics,
    inverse_roots,
    first_moment,
    second_moment,
):
    f32, bf16 = jnp.float32, jnp.bfloat16
    width = activations.shape[1]
    groups = output_grads.shape[1]
    replicas = lax.axis_size("replica")
    shards = lax.axis_size("shard")
    size = replicas // groups
    local_bits = range(bits_of(size))
    shard_bits = list(range(bits_of(shards)))[::-1]
    span = statistics.shape[0]
    replica = lax.axis_index("replica")
    slot, local = replica // size, replica % size
    shard = lax.axis_index("shard")
    span_index = local * shards + shard

    slot_ids = jnp.arange(groups, dtype=jnp.int32)
    onehot = (owner[None, :] == slot_ids[:, None]).astype(jnp.int32)
    source = jnp.sum(onehot * slot_ids[None, :], axis=1)

    order = [sorted(range(groups), key=lambda s: (-abs(s - z), s)) for z in range(groups)]
    block_order = jnp.take(source, jnp.take(jnp.asarray(np.array(order, np.int32)), slot, axis=0))
    douts = output_grads.transpose(1, 0, 2)
    rounds = []
    for k in range(groups):
        part = lax.dot_general(
            activations,
            lax.dynamic_index_in_dim(douts, block_order[k], 0, keepdims=False),
            (((0,), (0,)), ((), ())),
            preferred_element_type=f32,
        )
        for bit in list(local_bits)[::-1]:
            half = part.shape[0] // 2
            mine = (local >> bit) & 1
            away = lax.dynamic_slice_in_dim(part, (1 - mine) * half, half, 0).astype(bf16)
            part = lax.dynamic_slice_in_dim(part, mine * half, half, 0) + swap(
                away, "replica", bit
            ).astype(f32)
        rounds.append(part)

    def shift(value, up, senders):
        step = size if up else -size
        return lax.ppermute(
            value,
            "replica",
            [(r, r + step) for r in range(replicas) if r // size in senders],
        )

    came_up = came_down = None
    for t in range(1, groups):
        ups = {z: order[z].index(groups - t + z) for z in range(t)}
        downs = {z: order[z].index(z + t - groups) for z in range(groups - t, groups)}
        up = choose(rounds, ups, slot)
        down = choose(rounds, downs, slot)
        if came_up is not None:
            up = up + came_up.astype(f32)
            down = down + came_down.astype(f32)
        came_up = shift(up.astype(bf16), True, ups)
        came_down = shift(down.astype(bf16), False, downs)
    own = (rounds[-1] + came_up.astype(f32) + came_down.astype(f32)).astype(bf16)

    rows = own.shape[0]
    top, low = own[: rows // 2], own[rows // 2 :]
    for bit in local_bits:
        top = double(top, "replica", bit, 0)
    for bit in shard_bits[:-1]:
        low = double(low, "shard", bit, 1)
        top = double(top, "shard", bit, 1)
    for bit in local_bits:
        low = double(low, "replica", bit, 0)
    for bit in shard_bits[-1:]:
        low = double(low, "shard", bit, 1)
        top = double(top, "shard", bit, 1)
    pieces = []
    for k in range(size):
        for half in (top, low):
            pieces.append(lax.slice_in_dim(half, k * (rows // 2), (k + 1) * (rows // 2), axis=0))
    full_grad = reorder(jnp.concatenate(pieces, 0), shards, 1)

    left_root = inverse_roots[:, 0, :]
    for bit in shard_bits:
        left_root = double(left_root, "shard", bit, 0)
    left_root = reorder(left_root, shards, 0)
    pairs = []
    for r in range(replicas):
        for s in range(shards):
            j = (r % size) * shards + s
            target = (r // size * size + j % size) * shards + j // size
            pairs.append((r * shards + s, target))
    right_root = lax.ppermute(inverse_roots[:, 1, :], ("replica", "shard"), pairs)
    for bit in local_bits:
        right_root = double(right_root, "replica", bit, 0)

    right_part = lax.dot_general(
        full_grad, right_root, (((1,), (1,)), ((), ())), preferred_element_type=f32
    )
    high = lax.reduce_precision(right_part, 8, 7)
    rest = right_part - high
    precond = jnp.dot(left_root, high.astype(bf16), preferred_element_type=f32) + jnp.dot(
        left_root, rest.astype(bf16), preferred_element_type=f32
    )

    rounded = lax.dynamic_slice_in_dim(full_grad, span_index * span, span, 0)
    exact = rounded.astype(f32)
    count_float = step_count[0].astype(f32)
    first_new = beta_first * first_moment + (1.0 - beta_first) * exact
    second_new = beta_second * second_moment + (1.0 - beta_second) * exact * exact
    first_hat = first_new / (1.0 - jnp.power(beta_first, count_float))
    second_hat = second_new / (1.0 - jnp.power(beta_second, count_float))
    adam_dir = first_hat / (jnp.sqrt(second_hat) + eps_adam)

    sums = jnp.stack([jnp.sum(adam_dir * adam_dir), jnp.sum(precond * precond)])
    sums = jnp.broadcast_to(sums[:, None], (2, 128))
    for bit in local_bits:
        sums = sums + swap(sums, "replica", bit)
    for bit in shard_bits:
        sums = sums + swap(sums, "shard", bit)
    scale = jnp.sqrt(sums[0, 0]) / (jnp.sqrt(sums[1, 0]) + eps_norm)
    grafted = (precond * scale).astype(bf16)

    def complete(value, zs):
        for bit in local_bits:
            value = double(value, "replica", bit, 0, lambda r: r // size in zs)
        return value

    whole = {0: complete(grafted, range(groups))}
    up = down = grafted
    ups, downs = {}, {}
    for t in range(1, groups):
        up = shift(up, True, range(t - 1, groups - 1))
        down = shift(down, False, range(1, groups - t + 1))
        ups[t] = complete(up, range(t, groups))
        downs[t] = complete(down, range(0, groups - t))
    for m in range(1, groups):
        whole[m] = jnp.where(slot + m < groups, downs[m], ups[groups - m])
    update = jnp.zeros((groups,) + whole[0].shape, bf16)
    for m in range(groups):
        block = jnp.take(source, (slot + m) % groups)
        update = lax.dynamic_update_index_in_dim(update, whole[m], block, 0)

    grad_columns = lax.dynamic_slice_in_dim(full_grad, span_index * span, span, 1)
    left_gram = lax.dot_general(
        rounded, full_grad, (((1,), (1,)), ((), ())), preferred_element_type=f32
    )
    right_gram = lax.dot_general(
        grad_columns, full_grad, (((0,), (0,)), ((), ())), preferred_element_type=f32
    )
    new_left = beta_stat * statistics[:, 0, :] + (1.0 - beta_stat) * left_gram
    new_right = beta_stat * statistics[:, 1, :] + (1.0 - beta_stat) * right_gram
    new_stats = jnp.stack([new_left, new_right], axis=1)
    return (new_stats, first_new, second_new, update)


PARTS = 3
PIECES = 6


def is_equal(a, b):
    return lax.div(jnp.int32(1), 1 + (a - b) * (a - b))


def block_orders(groups):
    return [sorted(range(groups), key=lambda s: (-abs(s - z), s)) for z in range(groups)]


def power(base, count):
    out = jnp.float32(1.0)
    for bit in range(16):
        odd = lax.rem(lax.div(count, jnp.int32(1 << bit)), jnp.int32(2)) == 1
        out = out * jnp.where(odd, jnp.float32(base ** (1 << bit)), jnp.float32(1.0))
    return out


def step_kernel(
    groups,
    owner_ref,
    count_ref,
    a_hbm,
    d_hbm,
    roots_hbm,
    first_hbm,
    second_hbm,
    stats_hbm,
    update_hbm,
    first_out,
    second_out,
    stats_out,
    a,
    at,
    d,
    acc,
    away0,
    x_send,
    x_recv,
    z_send,
    up_recv,
    down_recv,
    p_send,
    p_recv,
    g,
    left,
    right,
    stage,
    roots,
    high,
    low,
    precond,
    first,
    second,
    columns,
    stats,
    u,
    norms,
    load_sem,
    out_sem,
    u_out_sem,
    x_ssem,
    x_rsem,
    p_ssem,
    p_rsem,
    z_ssem,
    up_rsem,
    down_rsem,
    g_ssem,
    g_rsem,
    l_ssem,
    l_rsem,
    r_ssem,
    r_rsem,
    n_ssem,
    n_rsem,
    ux_ssem,
    ux_rsem,
    uz_ssem,
    uu_rsem,
    ud_rsem,
):
    f32, bf16 = jnp.float32, jnp.bfloat16
    Z, Q, U = groups, PARTS, PIECES
    own = Z - 1
    width = g.shape[0]
    half = width // 2
    rows = half // Q
    cols = d.shape[2]
    span = first.shape[0]
    replica, s = lax.axis_index("replica"), lax.axis_index("shard")
    z, x = lax.div(replica, 2), lax.rem(replica, 2)
    y, c = lax.div(s, 2), lax.rem(s, 2)
    i = x * 4 + s
    x_dev = (z * 2 + 1 - x, s)
    y_dev = (replica, (1 - y) * 2 + c)
    c_dev = (replica, y * 2 + 1 - c)
    up_dev = (replica + 2, s)
    down_dev = (replica - 2, s)

    def remote(src, dst, ssem, rsem, dev):
        return pltpu.make_async_remote_copy(
            src_ref=src,
            dst_ref=dst,
            send_sem=ssem,
            recv_sem=rsem,
            device_id=dev,
            device_id_type=pl.DeviceIdType.MESH,
        )

    def peer(k):
        j = lax.rem(i + k, 8)
        return (z * 2 + lax.div(j, 4), lax.rem(j, 4))

    loads = [
        pltpu.make_async_copy(a_hbm, a, load_sem.at[0]),
        pltpu.make_async_copy(d_hbm, d, load_sem.at[1]),
        pltpu.make_async_copy(roots_hbm, roots, load_sem.at[2]),
        pltpu.make_async_copy(first_hbm, first, load_sem.at[3]),
        pltpu.make_async_copy(second_hbm, second, load_sem.at[4]),
        pltpu.make_async_copy(stats_hbm, stats, load_sem.at[5]),
    ]
    loads[0].start()
    loads[1].start()

    barrier = pltpu.get_barrier_semaphore()

    def greet(dev):
        pl.semaphore_signal(barrier, inc=1, device_id=dev, device_id_type=pl.DeviceIdType.MESH)

    for k in range(1, 8):
        greet(peer(k))
    has_below, has_above = z > 0, z < Z - 1

    @pl.when(has_above)
    def _():
        greet(up_dev)

    @pl.when(has_below)
    def _():
        greet(down_dev)

    for load in loads[2:]:
        load.start()
    loads[0].wait()
    orders = block_orders(Z)

    def target(k):
        return sum(
            is_equal(z, p) * is_equal(k, q) * orders[p][q] for p in range(Z) for q in range(Z)
        )

    def x_copy(k, q):
        return remote(x_send.at[k, q], x_recv.at[k, q], x_ssem.at[k, q], x_rsem.at[k, q], x_dev)

    def up_copy(k, m, t):
        return remote(z_send.at[k, m], up_recv.at[t, m], z_ssem.at[k, m], up_rsem.at[t, m], up_dev)

    def down_copy(k, m, t):
        return remote(
            z_send.at[k, m], down_recv.at[t, m], z_ssem.at[k, m], down_rsem.at[t, m], down_dev
        )

    def gather(ref, k, m, t, from_below, from_above):
        @pl.when(from_below)
        def _():
            up_copy(k, m, t).wait_recv()
            ref[...] = ref[...] + up_recv[t, m].astype(f32)

        @pl.when(from_above)
        def _():
            down_copy(k, m, t).wait_recv()
            ref[...] = ref[...] + down_recv[t, m].astype(f32)

    def pass_on(ref, k, m):
        t = target(k)
        gather(ref, k, m, t, (t > z) & has_below, (t < z) & has_above)
        z_send[k, m] = ref[...].astype(bf16)

        @pl.when(t > z)
        def _():
            up_copy(k, m, t).start()

        @pl.when(t < z)
        def _():
            down_copy(k, m, t).start()

    def multiply(k, carry):
        t = target(k)
        block = jnp.int32(0)
        for b in range(Z):
            block = jnp.where(owner_ref[b] == t, jnp.int32(b), block)

        def product(side, q):
            r = pl.ds(pl.multiple_of(side * half + q * rows, rows), rows)

            @pl.when(k == 0)
            def _():
                at[r, :] = a[:, r].T

            return jnp.dot(at[r, :], d[block], preferred_element_type=f32)

        def send_away(q, carry):
            x_send[k, q - 1] = product(1 - x, q).astype(bf16)
            x_copy(k, q - 1).start()
            return carry

        def keep(q, carry):
            acc[k, q] = product(x, q)
            return carry

        lax.fori_loop(1, Q, send_away, 0)
        away0[k] = product(1 - x, 0)
        lax.fori_loop(0, Q, keep, 0)

        @pl.when(k > 0)
        def _():
            pass_on(acc.at[k - 1, 0], k - 1, 0)
            pass_on(away0.at[k - 1], k - 1, Q)

        return carry

    loads[1].wait()
    pl.semaphore_wait(barrier, 9 - is_equal(z, 0) - is_equal(z, Z - 1))
    lax.fori_loop(0, Z, multiply, 0)

    def left_rows(shard):
        return left.at[pl.ds(pl.multiple_of(shard * span, span), span)]

    loads[2].wait()
    stage[...] = roots[:, 1, :]
    place = right.at[pl.ds(pl.multiple_of(c * span, span), span)]
    at_home = is_equal(x, y) * is_equal(y, c)

    def r_copy(tx):
        return remote(stage, place, r_ssem.at[tx], r_rsem.at[c], (z * 2 + tx, x * 2 + y))

    for tx in range(2):

        @pl.when(is_equal(x, tx) * at_home == 0)
        def _(tx=tx):
            r_copy(tx).start()

    @pl.when(at_home == 1)
    def _():
        place[...] = stage[...]

    left_rows(s)[...] = roots[:, 0, :]
    s_y = (1 - y) * 2 + c
    l_y = remote(left_rows(s), left_rows(s), l_ssem.at[0], l_rsem.at[0], y_dev)
    l_c = remote(left_rows(s), left_rows(s), l_ssem.at[1], l_rsem.at[1], c_dev)
    l_f = remote(left_rows(s_y), left_rows(s_y), l_ssem.at[2], l_rsem.at[2], c_dev)
    l_y.start()
    l_c.start()

    def pass_reduced(n, carry):
        k, q = lax.div(n, Q - 1), lax.rem(n, Q - 1)
        x_copy(k, q).wait_recv()
        acc[k, q + 1] = acc[k, q + 1] + x_recv[k, q].astype(f32)
        pass_on(acc.at[k, q + 1], k, q + 1)
        return carry

    lax.fori_loop(0, (Z - 1) * (Q - 1), pass_reduced, 0)
    l_y.wait_recv()
    l_f.start()

    def p_copy(m):
        return remote(p_send.at[m], p_recv.at[m], p_ssem.at[m], p_rsem.at[m], x_dev)

    for m in (0, Q) + tuple(range(1, Q)):
        ref = away0.at[own] if m == Q else acc.at[own, m]
        gather(ref, own, m, z, has_below, has_above)
        p_send[m] = ref[...].astype(bf16)
        p_copy(m).start()

    def tile(cc, shard):
        top = pl.multiple_of(cc * rows, rows)
        side = pl.multiple_of(shard * cols, cols)
        return g.at[pl.ds(top, rows), pl.ds(side, cols)]

    def g_copy(rel, cc):
        ref = tile(cc, s_y if rel == 2 else s)
        dev = y_dev if rel == 1 else c_dev
        return remote(ref, ref, g_ssem.at[rel, cc], g_rsem.at[rel, cc], dev)

    plan = [(0, q) for q in range(1, Q)] + [(0, 0)] + [(1, q) for q in range(Q)]

    def chunk(j):
        side, q = plan[j]
        return (x if side == 0 else 1 - x) * Q + q

    def put(j):
        side, q = plan[j]
        if side == 0 and q > 0:
            x_copy(own, q - 1).wait_recv()
            value = acc[own, q] + x_recv[own, q - 1].astype(f32)
        elif side == 0:
            p_copy(Q).wait_recv()
            value = acc[own, 0] + p_recv[Q].astype(f32)
        elif q == 0:
            p_copy(0).wait_recv()
            value = away0[own] + p_recv[0].astype(f32)
        else:
            p_copy(q).wait_recv()
            value = x_send[own, q - 1].astype(f32) + p_recv[q].astype(f32)
        cc = chunk(j)
        tile(cc, s)[...] = value.astype(bf16)
        g_copy(1, cc).start()
        g_copy(0, cc).start()

    def forward(j):
        g_copy(1, chunk(j)).wait_recv()
        g_copy(2, chunk(j)).start()

    def precondition(j):
        cc = chunk(j)
        g_copy(0, cc).wait_recv()
        g_copy(2, cc).wait_recv()
        r = pl.ds(pl.multiple_of(cc * rows, rows), rows)
        value = lax.dot_general(
            g[r, :], right[...], (((1,), (1,)), ((), ())), preferred_element_type=f32
        )
        top = value.astype(bf16)
        high[...] = top
        low[...] = (value - top.astype(f32)).astype(bf16)

        def times_left(n, carry):
            o = pl.ds(pl.multiple_of(n * rows, rows), rows)
            value = jnp.dot(left[o, r], high[...], preferred_element_type=f32) + jnp.dot(
                left[o, r], low[...], preferred_element_type=f32
            )
            precond[o, :] = value if j == 0 else precond[o, :] + value
            return carry

        lax.fori_loop(0, Q, times_left, 0)

    base = pl.multiple_of(i * span, span)
    lot = 16

    def adam(n, carry):
        total, first_bias, second_bias = carry
        r = pl.ds(pl.multiple_of(n * lot, lot), lot)
        grad = g[pl.ds(pl.multiple_of(base + n * lot, lot), lot), :].astype(f32)
        first_new = beta_first * first[r, :] + (1.0 - beta_first) * grad
        second_new = beta_second * second[r, :] + (1.0 - beta_second) * grad * grad
        first[r, :] = first_new
        second[r, :] = second_new
        value = (first_new * first_bias) / (jnp.sqrt(second_new * second_bias) + eps_adam)
        return total + value * value, first_bias, second_bias

    outs = [
        pltpu.make_async_copy(first, first_out, out_sem.at[0]),
        pltpu.make_async_copy(second, second_out, out_sem.at[1]),
        pltpu.make_async_copy(stats, stats_out, out_sem.at[2]),
    ]
    last = len(plan)
    adam_squares = None
    for j in range(last + 2):
        if j < last:
            put(j)
        if 1 <= j <= last:
            forward(j - 1)
        if j == 2:
            for rc in range(2):

                @pl.when(at_home * is_equal(c, rc) == 0)
                def _(rc=rc):
                    remote(
                        stage, right.at[pl.ds(rc * span, span)], r_ssem.at[0], r_rsem.at[rc], x_dev
                    ).wait_recv()

            l_c.wait_recv()
            l_f.wait_recv()
        if j >= 2:
            precondition(j - 2)
        if j == Q + 1:
            for load in loads[3:]:
                load.wait()
            first_bias = 1.0 / jnp.full((1, width), 1.0 - power(beta_first, count_ref[0]))
            second_bias = 1.0 / jnp.full((1, width), 1.0 - power(beta_second, count_ref[0]))
            total, _, _ = lax.fori_loop(
                0, span // lot, adam, (jnp.zeros((lot, width), f32), first_bias, second_bias)
            )
            adam_squares = jnp.sum(total)
            outs[0].start()
            outs[1].start()

    def squares(n, total):
        value = precond[pl.ds(pl.multiple_of(n * lot, lot), lot), :]
        return total + value * value

    precond_squares = jnp.sum(
        lax.fori_loop(0, half // lot, squares, jnp.zeros((lot, cols), f32))
    )
    which = lax.broadcasted_iota(jnp.int32, norms.shape[1:], 0)
    norms[i] = jnp.where(which == 0, adam_squares, precond_squares)

    def n_copy(k):
        return remote(norms.at[i], norms.at[i], n_ssem.at[k - 1], n_rsem.at[i], peer(k))

    for k in range(1, 8):
        n_copy(k).start()
    for k in range(1, 8):
        j = lax.rem(i + k, 8)
        remote(norms.at[j], norms.at[j], n_ssem.at[k - 1], n_rsem.at[j], peer(k)).wait_recv()
    total = norms[0]
    for k in range(1, 8):
        total = total + norms[k]
    scale = jnp.sqrt(total[0:1, :]) / (jnp.sqrt(total[1:2, :]) + eps_norm)

    piece = half // U

    def part(zt, xt, q):
        top = pl.multiple_of(xt * half + q * piece, piece)
        return u.at[zt, pl.ds(top, piece), :]

    def z_part(zt, m):
        return part(zt, 1 - x, 0) if m == U else part(zt, x, m)

    def ux_copy(zt, q):
        return remote(part(zt, x, q), part(zt, x, q), ux_ssem.at[zt, q], ux_rsem.at[zt, q], x_dev)

    def uu_copy(zt, m):
        return remote(z_part(zt, m), z_part(zt, m), uz_ssem.at[0, zt, m], uu_rsem.at[zt, m], up_dev)

    def ud_copy(zt, m):
        return remote(z_part(zt, m), z_part(zt, m), uz_ssem.at[1, zt, m], ud_rsem.at[zt, m], down_dev)

    def store(zt, xt, q):
        top = pl.multiple_of(xt * half + q * piece, piece)
        return pltpu.make_async_copy(
            part(zt, xt, q), update_hbm.at[zt, pl.ds(top, piece), :], u_out_sem.at[zt, xt, q]
        )

    def spread(m):
        @pl.when(has_above)
        def _():
            uu_copy(z, m).start()

        @pl.when(has_below)
        def _():
            ud_copy(z, m).start()

    for q in range(U):
        part(z, x, q)[...] = (precond[pl.ds(q * piece, piece), :] * scale).astype(bf16)
        ux_copy(z, q).start()
        spread(q)
        store(z, x, q).start()
    ux_copy(z, 0).wait_recv()
    spread(U)
    store(z, 1 - x, 0).start()

    window = pl.multiple_of(lax.div(i, 2) * cols, cols)
    turned = g[:, pl.ds(window, cols)].T
    columns[...] = jnp.where(lax.rem(i, 2) == 1, turned[span:, :], turned[:span, :])

    def grams(n, carry):
        r = pl.ds(pl.multiple_of(n * cols, cols), cols)
        left_gram = lax.dot_general(
            g[pl.ds(base, span), :], g[r, :], (((1,), (1,)), ((), ())), preferred_element_type=f32
        )
        stats[:, 0, r] = beta_stat * stats[:, 0, r] + (1.0 - beta_stat) * left_gram
        right_gram = jnp.dot(columns[...], g[:, r], preferred_element_type=f32)
        stats[:, 1, r] = beta_stat * stats[:, 1, r] + (1.0 - beta_stat) * right_gram
        return carry

    lax.fori_loop(0, width // cols, grams, 0)
    outs[2].start()

    def relay(zt, m, copy, onward):
        copy(zt, m).wait_recv()

        @pl.when(onward)
        def _():
            copy(zt, m).start()

        if 0 < m < U:
            ux_copy(zt, m).start()
        store(zt, 1 - x if m == U else x, 0 if m == U else m).start()

    for dist in range(1, Z):

        @pl.when(z - dist >= 0)
        def _(dist=dist):
            relay(z - dist, 0, uu_copy, has_above)

        @pl.when(z + dist < Z)
        def _(dist=dist):
            relay(z + dist, 0, ud_copy, has_below)

        for m in range(1, U + 1):

            @pl.when(z - dist >= 0)
            def _(dist=dist, m=m):
                relay(z - dist, m, uu_copy, has_above)

            @pl.when(z + dist < Z)
            def _(dist=dist, m=m):
                relay(z + dist, m, ud_copy, has_below)

    def arrive(zt):
        for q in range(1, U):
            ux_copy(zt, q).wait_recv()
            store(zt, 1 - x, q).start()

    arrive(z)
    for dist in range(1, Z):

        @pl.when(z - dist >= 0)
        def _(dist=dist):
            arrive(z - dist)

        @pl.when(z + dist < Z)
        def _(dist=dist):
            arrive(z + dist)

    l_y.wait_send()
    l_c.wait_send()
    l_f.wait_send()
    for tx in range(2):

        @pl.when(is_equal(x, tx) * at_home == 0)
        def _(tx=tx):
            r_copy(tx).wait_send()

    for k in range(1, 8):
        n_copy(k).wait_send()

    def sent(k, carry):
        for q in range(Q - 1):
            x_copy(k, q).wait_send()

        @pl.when(k < Z - 1)
        def _():
            for m in range(Q + 1):
                up_copy(k, m, k).wait_send()

        ux_last = is_equal(k, z)

        @pl.when(ux_last == 1)
        def _():
            ux_copy(k, 0).wait_send()

        for q in range(1, U):
            ux_copy(k, q).wait_send()
        for q in range(U):
            store(k, 0, q).wait()
            store(k, 1, q).wait()

        @pl.when((z >= k) & has_above)
        def _():
            for m in range(U + 1):
                uu_copy(k, m).wait_send()

        @pl.when((z <= k) & has_below)
        def _():
            for m in range(U + 1):
                ud_copy(k, m).wait_send()

        return carry

    lax.fori_loop(0, Z, sent, 0)
    for m in range(Q + 1):
        p_copy(m).wait_send()
    for rel in range(3):
        for cc in range(2 * Q):
            g_copy(rel, cc).wait_send()
    for out in outs:
        out.wait()


def finish_kernel(
    owner_ref, update_in, first_in, second_in, stats_in, update, first, second, stats, u, f, s, t, isem, osem
):
    Z, half = u.shape[0], u.shape[1] // 2
    moves = []
    for b in range(Z):
        for h in range(2):
            r = pl.ds(h * half, half)
            moves.append((update_in.at[owner_ref[b], r, :], u.at[b, r, :], update.at[b, r, :]))
    moves += [(first_in, f, first), (second_in, s, second), (stats_in, t, stats)]
    ins = [pltpu.make_async_copy(m[0], m[1], isem.at[n]) for n, m in enumerate(moves)]
    outs = [pltpu.make_async_copy(m[1], m[2], osem.at[n]) for n, m in enumerate(moves)]
    for copy in ins:
        copy.start()
    for copy, out in zip(ins, outs):
        copy.wait()
        out.start()
    for out in outs:
        out.wait()


def fused_body(
    activations,
    output_grads,
    owner,
    step_count,
    statistics,
    inverse_roots,
    first_moment,
    second_moment,
):
    f32, bf16 = jnp.float32, jnp.bfloat16
    tokens, width = activations.shape
    groups, cols = output_grads.shape[1:]
    span = statistics.shape[0]
    half, Q, U = width // 2, PARTS, PIECES
    rows = half // Q

    VMEM, DMA = pltpu.VMEM, pltpu.SemaphoreType.DMA
    hbm = pl.BlockSpec(memory_space=pl.ANY)
    smem = pl.BlockSpec(memory_space=pltpu.SMEM)
    results = (
        jax.ShapeDtypeStruct((groups, width, cols), bf16),
        jax.ShapeDtypeStruct((span, width), f32),
        jax.ShapeDtypeStruct((span, width), f32),
        jax.ShapeDtypeStruct((span, 2, width), f32),
    )
    params = dict(vmem_limit_bytes=60 * 1024 * 1024)
    update, first_new, second_new, new_stats = pl.pallas_call(
        functools.partial(step_kernel, groups),
        out_shape=results,
        in_specs=[smem, smem] + [hbm] * 6,
        out_specs=[hbm] * 4,
        scratch_shapes=[
            VMEM((tokens, width), bf16),
            VMEM((width, tokens), bf16),
            VMEM((groups, tokens, cols), bf16),
            VMEM((groups, Q, rows, cols), f32),
            VMEM((groups, rows, cols), f32),
            VMEM((groups, Q - 1, rows, cols), bf16),
            VMEM((groups, Q - 1, rows, cols), bf16),
            VMEM((groups, Q + 1, rows, cols), bf16),
            VMEM((groups, Q + 1, rows, cols), bf16),
            VMEM((groups, Q + 1, rows, cols), bf16),
            VMEM((Q + 1, rows, cols), bf16),
            VMEM((Q + 1, rows, cols), bf16),
            VMEM((width, width), bf16),
            VMEM((half, width), bf16),
            VMEM((2 * span, width), bf16),
            VMEM((span, width), bf16),
            VMEM((span, 2, width), bf16),
            VMEM((rows, cols), bf16),
            VMEM((rows, cols), bf16),
            VMEM((half, cols), f32),
            VMEM((span, width), f32),
            VMEM((span, width), f32),
            VMEM((span, width), bf16),
            VMEM((span, 2, width), f32),
            VMEM((groups, width, cols), bf16),
            VMEM((8, 8, cols), f32),
            DMA((6,)),
            DMA((3,)),
            DMA((groups, 2, U)),
            DMA((groups, Q - 1)),
            DMA((groups, Q - 1)),
            DMA((Q + 1,)),
            DMA((Q + 1,)),
            DMA((groups, Q + 1)),
            DMA((groups, Q + 1)),
            DMA((groups, Q + 1)),
            DMA((3, 2 * Q)),
            DMA((3, 2 * Q)),
            DMA((3,)),
            DMA((3,)),
            DMA((2,)),
            DMA((2,)),
            DMA((7,)),
            DMA((8,)),
            DMA((groups, U)),
            DMA((groups, U)),
            DMA((2, groups, U + 1)),
            DMA((groups, U + 1)),
            DMA((groups, U + 1)),
        ],
        compiler_params=pltpu.CompilerParams(collective_id=0, has_side_effects=True, **params),
        name="step_kernel",
    )(
        owner,
        step_count,
        activations,
        output_grads.transpose(1, 0, 2),
        inverse_roots,
        first_moment,
        second_moment,
        statistics,
    )
    moves = 2 * groups + 3
    update, first_new, second_new, new_stats = pl.pallas_call(
        finish_kernel,
        out_shape=results,
        in_specs=[smem] + [hbm] * 4,
        out_specs=[hbm] * 4,
        scratch_shapes=[VMEM(r.shape, r.dtype) for r in results] + [DMA((moves,)), DMA((moves,))],
        compiler_params=pltpu.CompilerParams(**params),
        name="finish_kernel",
    )(owner, update, first_new, second_new, new_stats)
    return (new_stats, first_new, second_new, update)


def dispatch(replicas, shards, *args):
    width, groups, cols = args[0].shape[1], args[1].shape[1], args[1].shape[2]
    whole = width % (256 * PARTS) == 0 and width % (256 * PIECES) == 0 and cols % 128 == 0
    if replicas == 2 * groups and shards == 4 and whole:
        return fused_body(*args)
    return body(*args)


def solution(mesh):
    placed = (
        P("replica", None),
        P("replica", None, "shard"),
        P(),
        P(),
        P(("replica", "shard"), None, None),
        P(("replica", "shard"), None, None),
        P(("replica", "shard"), None),
        P(("replica", "shard"), None),
    )
    return jax.shard_map(
        functools.partial(dispatch, mesh.shape["replica"], mesh.shape["shard"]),
        mesh=mesh,
        in_specs=placed,
        out_specs=(
            P(("replica", "shard"), None, None),
            P(("replica", "shard"), None),
            P(("replica", "shard"), None),
            P(None, None, "shard"),
        ),
        check_vma=False,
    )
```

```python
import functools

import jax
import jax.numpy as jnp
import numpy as np
from jax import lax
from jax.experimental import pallas as pl
from jax.experimental.pallas import tpu as pltpu
from jax.sharding import PartitionSpec as P

beta_stat = 0.9
beta_first = 0.9
beta_second = 0.999
eps_adam = 1e-08
eps_norm = 1e-06


def bits_of(extent):
    return extent.bit_length() - 1


def swap(value, axis, bit, keep=lambda i: True):
    n = lax.axis_size(axis)
    return lax.ppermute(value, axis, [(i, i ^ (1 << bit)) for i in range(n) if keep(i)])


def join(value, partner, axis, bit, dim):
    upper = (lax.axis_index(axis) >> bit) & 1 == 1
    return jnp.where(
        upper,
        jnp.concatenate([partner, value], dim),
        jnp.concatenate([value, partner], dim),
    )


def double(value, axis, bit, dim, keep=lambda i: True):
    return join(value, swap(value, axis, bit, keep), axis, bit, dim)


def reversed_bits(count):
    bits = bits_of(count)
    return [int(format(i, "b").zfill(bits)[::-1], 2) if bits else 0 for i in range(count)]


def reorder(value, count, dim):
    size = value.shape[dim] // count
    return jnp.concatenate(
        [lax.slice_in_dim(value, k * size, (k + 1) * size, axis=dim) for k in reversed_bits(count)],
        dim,
    )


def choose(values, picks, slot):
    out = values[picks[max(picks)]]
    for z in sorted(picks):
        if values[picks[z]] is not out:
            out = jnp.where(slot == z, values[picks[z]], out)
    return out


def body(
    activations,
    output_grads,
    owner,
    step_count,
    statistics,
    inverse_roots,
    first_moment,
    second_moment,
):
    f32, bf16 = jnp.float32, jnp.bfloat16
    width = activations.shape[1]
    groups = output_grads.shape[1]
    replicas = lax.axis_size("replica")
    shards = lax.axis_size("shard")
    size = replicas // groups
    local_bits = range(bits_of(size))
    shard_bits = list(range(bits_of(shards)))[::-1]
    span = statistics.shape[0]
    replica = lax.axis_index("replica")
    slot, local = replica // size, replica % size
    shard = lax.axis_index("shard")
    span_index = local * shards + shard

    slot_ids = jnp.arange(groups, dtype=jnp.int32)
    onehot = (owner[None, :] == slot_ids[:, None]).astype(jnp.int32)
    source = jnp.sum(onehot * slot_ids[None, :], axis=1)

    order = [sorted(range(groups), key=lambda s: (-abs(s - z), s)) for z in range(groups)]
    block_order = jnp.take(source, jnp.take(jnp.asarray(np.array(order, np.int32)), slot, axis=0))
    douts = output_grads.transpose(1, 0, 2)
    rounds = []
    for k in range(groups):
        part = lax.dot_general(
            activations,
            lax.dynamic_index_in_dim(douts, block_order[k], 0, keepdims=False),
            (((0,), (0,)), ((), ())),
            preferred_element_type=f32,
        )
        for bit in list(local_bits)[::-1]:
            half = part.shape[0] // 2
            mine = (local >> bit) & 1
            away = lax.dynamic_slice_in_dim(part, (1 - mine) * half, half, 0).astype(bf16)
            part = lax.dynamic_slice_in_dim(part, mine * half, half, 0) + swap(
                away, "replica", bit
            ).astype(f32)
        rounds.append(part)

    def shift(value, up, senders):
        step = size if up else -size
        return lax.ppermute(
            value,
            "replica",
            [(r, r + step) for r in range(replicas) if r // size in senders],
        )

    came_up = came_down = None
    for t in range(1, groups):
        ups = {z: order[z].index(groups - t + z) for z in range(t)}
        downs = {z: order[z].index(z + t - groups) for z in range(groups - t, groups)}
        up = choose(rounds, ups, slot)
        down = choose(rounds, downs, slot)
        if came_up is not None:
            up = up + came_up.astype(f32)
            down = down + came_down.astype(f32)
        came_up = shift(up.astype(bf16), True, ups)
        came_down = shift(down.astype(bf16), False, downs)
    own = (rounds[-1] + came_up.astype(f32) + came_down.astype(f32)).astype(bf16)

    rows = own.shape[0]
    top, low = own[: rows // 2], own[rows // 2 :]
    for bit in local_bits:
        top = double(top, "replica", bit, 0)
    for bit in shard_bits[:-1]:
        low = double(low, "shard", bit, 1)
        top = double(top, "shard", bit, 1)
    for bit in local_bits:
        low = double(low, "replica", bit, 0)
    for bit in shard_bits[-1:]:
        low = double(low, "shard", bit, 1)
        top = double(top, "shard", bit, 1)
    pieces = []
    for k in range(size):
        for half in (top, low):
            pieces.append(lax.slice_in_dim(half, k * (rows // 2), (k + 1) * (rows // 2), axis=0))
    full_grad = reorder(jnp.concatenate(pieces, 0), shards, 1)

    left_root = inverse_roots[:, 0, :]
    for bit in shard_bits:
        left_root = double(left_root, "shard", bit, 0)
    left_root = reorder(left_root, shards, 0)
    pairs = []
    for r in range(replicas):
        for s in range(shards):
            j = (r % size) * shards + s
            target = (r // size * size + j % size) * shards + j // size
            pairs.append((r * shards + s, target))
    right_root = lax.ppermute(inverse_roots[:, 1, :], ("replica", "shard"), pairs)
    for bit in local_bits:
        right_root = double(right_root, "replica", bit, 0)

    right_part = lax.dot_general(
        full_grad, right_root, (((1,), (1,)), ((), ())), preferred_element_type=f32
    )
    high = lax.reduce_precision(right_part, 8, 7)
    rest = right_part - high
    precond = jnp.dot(left_root, high.astype(bf16), preferred_element_type=f32) + jnp.dot(
        left_root, rest.astype(bf16), preferred_element_type=f32
    )

    rounded = lax.dynamic_slice_in_dim(full_grad, span_index * span, span, 0)
    exact = rounded.astype(f32)
    count_float = step_count[0].astype(f32)
    first_new = beta_first * first_moment + (1.0 - beta_first) * exact
    second_new = beta_second * second_moment + (1.0 - beta_second) * exact * exact
    first_hat = first_new / (1.0 - jnp.power(beta_first, count_float))
    second_hat = second_new / (1.0 - jnp.power(beta_second, count_float))
    adam_dir = first_hat / (jnp.sqrt(second_hat) + eps_adam)

    sums = jnp.stack([jnp.sum(adam_dir * adam_dir), jnp.sum(precond * precond)])
    sums = jnp.broadcast_to(sums[:, None], (2, 128))
    for bit in local_bits:
        sums = sums + swap(sums, "replica", bit)
    for bit in shard_bits:
        sums = sums + swap(sums, "shard", bit)
    scale = jnp.sqrt(sums[0, 0]) / (jnp.sqrt(sums[1, 0]) + eps_norm)
    grafted = (precond * scale).astype(bf16)

    def complete(value, zs):
        for bit in local_bits:
            value = double(value, "replica", bit, 0, lambda r: r // size in zs)
        return value

    whole = {0: complete(grafted, range(groups))}
    up = down = grafted
    ups, downs = {}, {}
    for t in range(1, groups):
        up = shift(up, True, range(t - 1, groups - 1))
        down = shift(down, False, range(1, groups - t + 1))
        ups[t] = complete(up, range(t, groups))
        downs[t] = complete(down, range(0, groups - t))
    for m in range(1, groups):
        whole[m] = jnp.where(slot + m < groups, downs[m], ups[groups - m])
    update = jnp.zeros((groups,) + whole[0].shape, bf16)
    for m in range(groups):
        block = jnp.take(source, (slot + m) % groups)
        update = lax.dynamic_update_index_in_dim(update, whole[m], block, 0)

    grad_columns = lax.dynamic_slice_in_dim(full_grad, span_index * span, span, 1)
    left_gram = lax.dot_general(
        rounded, full_grad, (((1,), (1,)), ((), ())), preferred_element_type=f32
    )
    right_gram = lax.dot_general(
        grad_columns, full_grad, (((0,), (0,)), ((), ())), preferred_element_type=f32
    )
    new_left = beta_stat * statistics[:, 0, :] + (1.0 - beta_stat) * left_gram
    new_right = beta_stat * statistics[:, 1, :] + (1.0 - beta_stat) * right_gram
    new_stats = jnp.stack([new_left, new_right], axis=1)
    return (new_stats, first_new, second_new, update)


PARTS = 3
PIECES = 6


def is_equal(a, b):
    return lax.div(jnp.int32(1), 1 + (a - b) * (a - b))


def block_orders(groups):
    return [sorted(range(groups), key=lambda s: (-abs(s - z), s)) for z in range(groups)]


def power(base, count):
    out = jnp.float32(1.0)
    for bit in range(16):
        odd = lax.rem(lax.div(count, jnp.int32(1 << bit)), jnp.int32(2)) == 1
        out = out * jnp.where(odd, jnp.float32(base ** (1 << bit)), jnp.float32(1.0))
    return out


def step_kernel(
    groups,
    owner_ref,
    count_ref,
    a_hbm,
    d_hbm,
    roots_hbm,
    first_hbm,
    second_hbm,
    stats_hbm,
    update_hbm,
    first_out,
    second_out,
    stats_out,
    a,
    at,
    d,
    acc,
    away0,
    x_send,
    x_recv,
    z_send,
    up_recv,
    down_recv,
    p_send,
    p_recv,
    g,
    left,
    right,
    stage,
    roots,
    high,
    low,
    precond,
    first,
    second,
    columns,
    stats,
    u,
    norms,
    load_sem,
    out_sem,
    u_out_sem,
    x_ssem,
    x_rsem,
    p_ssem,
    p_rsem,
    z_ssem,
    up_rsem,
    down_rsem,
    g_ssem,
    g_rsem,
    l_ssem,
    l_rsem,
    r_ssem,
    r_rsem,
    n_ssem,
    n_rsem,
    ux_ssem,
    ux_rsem,
    uz_ssem,
    uu_rsem,
    ud_rsem,
):
    f32, bf16 = jnp.float32, jnp.bfloat16
    Z, Q, U = groups, PARTS, PIECES
    own = Z - 1
    width = g.shape[0]
    half = width // 2
    rows = half // Q
    cols = d.shape[2]
    span = first.shape[0]
    replica, s = lax.axis_index("replica"), lax.axis_index("shard")
    z, x = lax.div(replica, 2), lax.rem(replica, 2)
    y, c = lax.div(s, 2), lax.rem(s, 2)
    i = x * 4 + s
    x_dev = (z * 2 + 1 - x, s)
    y_dev = (replica, (1 - y) * 2 + c)
    c_dev = (replica, y * 2 + 1 - c)
    up_dev = (replica + 2, s)
    down_dev = (replica - 2, s)

    def remote(src, dst, ssem, rsem, dev):
        return pltpu.make_async_remote_copy(
            src_ref=src,
            dst_ref=dst,
            send_sem=ssem,
            recv_sem=rsem,
            device_id=dev,
            device_id_type=pl.DeviceIdType.MESH,
        )

    def peer(k):
        j = lax.rem(i + k, 8)
        return (z * 2 + lax.div(j, 4), lax.rem(j, 4))

    loads = [
        pltpu.make_async_copy(a_hbm, a, load_sem.at[0]),
        pltpu.make_async_copy(d_hbm, d, load_sem.at[1]),
        pltpu.make_async_copy(roots_hbm, roots, load_sem.at[2]),
        pltpu.make_async_copy(first_hbm, first, load_sem.at[3]),
        pltpu.make_async_copy(second_hbm, second, load_sem.at[4]),
        pltpu.make_async_copy(stats_hbm, stats, load_sem.at[5]),
    ]
    loads[0].start()
    loads[1].start()

    barrier = pltpu.get_barrier_semaphore()

    def greet(dev):
        pl.semaphore_signal(barrier, inc=1, device_id=dev, device_id_type=pl.DeviceIdType.MESH)

    for k in range(1, 8):
        greet(peer(k))
    has_below, has_above = z > 0, z < Z - 1

    @pl.when(has_above)
    def _():
        greet(up_dev)

    @pl.when(has_below)
    def _():
        greet(down_dev)

    for load in loads[2:]:
        load.start()
    loads[0].wait()
    orders = block_orders(Z)

    def target(k):
        return sum(
            is_equal(z, p) * is_equal(k, q) * orders[p][q] for p in range(Z) for q in range(Z)
        )

    def x_copy(k, q):
        return remote(x_send.at[k, q], x_recv.at[k, q], x_ssem.at[k, q], x_rsem.at[k, q], x_dev)

    def up_copy(k, m, t):
        return remote(z_send.at[k, m], up_recv.at[t, m], z_ssem.at[k, m], up_rsem.at[t, m], up_dev)

    def down_copy(k, m, t):
        return remote(
            z_send.at[k, m], down_recv.at[t, m], z_ssem.at[k, m], down_rsem.at[t, m], down_dev
        )

    def awaited(t):
        return (t > z) & has_below, (t < z) & has_above

    def gather(ref, k, m, t, from_below, from_above):
        @pl.when(from_below)
        def _():
            up_copy(k, m, t).wait_recv()
            ref[...] = ref[...] + up_recv[t, m].astype(f32)

        @pl.when(from_above)
        def _():
            down_copy(k, m, t).wait_recv()
            ref[...] = ref[...] + down_recv[t, m].astype(f32)

    def pass_on(ref, k, m):
        t = target(k)
        gather(ref, k, m, t, *awaited(t))
        z_send[k, m] = ref[...].astype(bf16)

        @pl.when(t > z)
        def _():
            up_copy(k, m, t).start()

        @pl.when(t < z)
        def _():
            down_copy(k, m, t).start()

    def left_rows(shard):
        return left.at[pl.ds(pl.multiple_of(shard * span, span), span)]

    place = right.at[pl.ds(pl.multiple_of(c * span, span), span)]
    at_home = is_equal(x, y) * is_equal(y, c)
    s_y = (1 - y) * 2 + c
    l_y = remote(left_rows(s), left_rows(s), l_ssem.at[0], l_rsem.at[0], y_dev)
    l_c = remote(left_rows(s), left_rows(s), l_ssem.at[1], l_rsem.at[1], c_dev)
    l_f = remote(left_rows(s_y), left_rows(s_y), l_ssem.at[2], l_rsem.at[2], c_dev)

    def r_copy(tx):
        return remote(stage, place, r_ssem.at[tx], r_rsem.at[c], (z * 2 + tx, x * 2 + y))

    def send_roots():
        loads[2].wait()
        stage[...] = roots[:, 1, :]
        for tx in range(2):

            @pl.when(is_equal(x, tx) * at_home == 0)
            def _(tx=tx):
                r_copy(tx).start()

        left_rows(s)[...] = roots[:, 0, :]
        l_y.start()
        l_c.start()

        @pl.when(at_home == 1)
        def _():
            place[...] = stage[...]

    def multiply(k, carry):
        t = target(k)
        block = jnp.int32(0)
        for b in range(Z):
            block = jnp.where(owner_ref[b] == t, jnp.int32(b), block)

        def product(side, q):
            r = pl.ds(pl.multiple_of(side * half + q * rows, rows), rows)

            @pl.when(k == 0)
            def _():
                at[r, :] = a[:, r].T

            return jnp.dot(at[r, :], d[block], preferred_element_type=f32)

        def send_away(q, carry):
            x_send[k, q - 1] = product(1 - x, q).astype(bf16)

            @pl.when(k < own - 1)
            def _():
                x_copy(k, q - 1).start()

            return carry

        def keep(q, carry):
            acc[k, q] = product(x, q)
            return carry

        from_below, from_above = awaited(t)
        waits = from_below | from_above

        def pass_first():
            pass_on(acc.at[k, 0], k, 0)
            pass_on(away0.at[k], k, Q)

        send_away(1, 0)
        keep(0, 0)
        away0[k] = product(1 - x, 0)

        @pl.when((k < own) & jnp.logical_not(waits))
        def _():
            pass_first()

        lax.fori_loop(2, Q, send_away, 0)
        lax.fori_loop(1, Q, keep, 0)

        @pl.when(k == 0)
        def _():
            send_roots()

        @pl.when((k < own) & waits)
        def _():
            pass_first()

        return carry

    loads[1].wait()
    pl.semaphore_wait(barrier, 9 - is_equal(z, 0) - is_equal(z, Z - 1))
    lax.fori_loop(0, Z, multiply, 0)

    def pass_reduced(n, carry):
        k, q = lax.div(n, Q - 1), lax.rem(n, Q - 1)
        x_copy(k, q).wait_recv()
        acc[k, q + 1] = acc[k, q + 1] + x_recv[k, q].astype(f32)
        pass_on(acc.at[k, q + 1], k, q + 1)
        return carry

    def p_copy(m):
        return remote(p_send.at[m], p_recv.at[m], p_ssem.at[m], p_rsem.at[m], x_dev)

    def own_sum(m):
        ref = away0.at[own] if m == Q else acc.at[own, m]
        gather(ref, own, m, z, has_below, has_above)
        p_send[m] = ref[...].astype(bf16)
        p_copy(m).start()

    def own_first():
        own_sum(0)
        own_sum(Q)
        for k in (own - 1, own):
            for q in range(Q - 1):
                x_copy(k, q).start()

    @pl.when(has_below & has_above)
    def _():
        own_first()

    lax.fori_loop(0, (own - 1) * (Q - 1), pass_reduced, 0)
    l_y.wait_recv()
    l_f.start()

    @pl.when(jnp.logical_not(has_below & has_above))
    def _():
        own_first()

    def tile(cc, shard):
        top = pl.multiple_of(cc * rows, rows)
        side = pl.multiple_of(shard * cols, cols)
        return g.at[pl.ds(top, rows), pl.ds(side, cols)]

    def g_copy(rel, cc):
        ref = tile(cc, s_y if rel == 2 else s)
        dev = y_dev if rel == 1 else c_dev
        return remote(ref, ref, g_ssem.at[rel, cc], g_rsem.at[rel, cc], dev)

    plan = [(0, 0), (1, 0)] + [(0, q) for q in range(1, Q)] + [(1, q) for q in range(1, Q)]

    def chunk(j):
        side, q = plan[j]
        return (x if side == 0 else 1 - x) * Q + q

    def put(j):
        side, q = plan[j]
        if side == 0 and q > 0:
            own_sum(q)
            x_copy(own, q - 1).wait_recv()
            value = acc[own, q] + x_recv[own, q - 1].astype(f32)
        elif side == 0:
            p_copy(Q).wait_recv()
            value = acc[own, 0] + p_recv[Q].astype(f32)
        elif q == 0:
            p_copy(0).wait_recv()
            value = away0[own] + p_recv[0].astype(f32)
        else:
            p_copy(q).wait_recv()
            value = x_send[own, q - 1].astype(f32) + p_recv[q].astype(f32)
        cc = chunk(j)
        tile(cc, s)[...] = value.astype(bf16)
        g_copy(1, cc).start()
        g_copy(0, cc).start()

    def forward(j):
        g_copy(1, chunk(j)).wait_recv()
        g_copy(2, chunk(j)).start()

    def precondition(j):
        cc = chunk(j)
        g_copy(0, cc).wait_recv()
        g_copy(2, cc).wait_recv()
        r = pl.ds(pl.multiple_of(cc * rows, rows), rows)
        value = lax.dot_general(
            g[r, :], right[...], (((1,), (1,)), ((), ())), preferred_element_type=f32
        )
        top = value.astype(bf16)
        high[...] = top
        low[...] = (value - top.astype(f32)).astype(bf16)

        def times_left(n, carry):
            o = pl.ds(pl.multiple_of(n * rows, rows), rows)
            value = jnp.dot(left[o, r], high[...], preferred_element_type=f32) + jnp.dot(
                left[o, r], low[...], preferred_element_type=f32
            )
            precond[o, :] = value if j == 0 else precond[o, :] + value
            return carry

        lax.fori_loop(0, Q, times_left, 0)

    base = pl.multiple_of(i * span, span)
    lot = 16

    def adam(n, carry):
        total, first_bias, second_bias = carry
        r = pl.ds(pl.multiple_of(n * lot, lot), lot)
        grad = g[pl.ds(pl.multiple_of(base + n * lot, lot), lot), :].astype(f32)
        first_new = beta_first * first[r, :] + (1.0 - beta_first) * grad
        second_new = beta_second * second[r, :] + (1.0 - beta_second) * grad * grad
        first[r, :] = first_new
        second[r, :] = second_new
        value = (first_new * first_bias) / (jnp.sqrt(second_new * second_bias) + eps_adam)
        return total + value * value, first_bias, second_bias

    outs = [
        pltpu.make_async_copy(first, first_out, out_sem.at[0]),
        pltpu.make_async_copy(second, second_out, out_sem.at[1]),
        pltpu.make_async_copy(stats, stats_out, out_sem.at[2]),
    ]
    def roots_here():
        for rc in range(2):

            @pl.when(at_home * is_equal(c, rc) == 0)
            def _(rc=rc):
                remote(
                    stage, right.at[pl.ds(rc * span, span)], r_ssem.at[0], r_rsem.at[rc], x_dev
                ).wait_recv()

        l_c.wait_recv()
        l_f.wait_recv()

    def adam_sum():
        for load in loads[3:]:
            load.wait()
        first_bias = 1.0 / jnp.full((1, width), 1.0 - power(beta_first, count_ref[0]))
        second_bias = 1.0 / jnp.full((1, width), 1.0 - power(beta_second, count_ref[0]))
        total, _, _ = lax.fori_loop(
            0, span // lot, adam, (jnp.zeros((lot, width), f32), first_bias, second_bias)
        )
        outs[0].start()
        outs[1].start()
        return jnp.sum(total)

    last = len(plan)
    for j in range(last):
        if j == 2:
            lax.fori_loop((own - 1) * (Q - 1), own * (Q - 1), pass_reduced, 0)
        put(j)
        if j >= 2:
            forward(j - 2)
        if j == 3:
            roots_here()
        if j >= 3:
            precondition(j - 3)
    forward(last - 2)
    precondition(last - 3)
    precondition(last - 2)
    forward(last - 1)
    adam_squares = adam_sum()
    precondition(last - 1)

    def squares(n, total):
        value = precond[pl.ds(pl.multiple_of(n * lot, lot), lot), :]
        return total + value * value

    precond_squares = jnp.sum(
        lax.fori_loop(0, half // lot, squares, jnp.zeros((lot, cols), f32))
    )
    which = lax.broadcasted_iota(jnp.int32, norms.shape[1:], 0)
    norms[i] = jnp.where(which == 0, adam_squares, precond_squares)

    def n_copy(k):
        return remote(norms.at[i], norms.at[i], n_ssem.at[k - 1], n_rsem.at[i], peer(k))

    for k in range(1, 8):
        n_copy(k).start()
    for k in range(1, 8):
        j = lax.rem(i + k, 8)
        remote(norms.at[j], norms.at[j], n_ssem.at[k - 1], n_rsem.at[j], peer(k)).wait_recv()
    total = norms[0]
    for k in range(1, 8):
        total = total + norms[k]
    scale = jnp.sqrt(total[0:1, :]) / (jnp.sqrt(total[1:2, :]) + eps_norm)

    piece = half // U

    def part(zt, xt, q):
        top = pl.multiple_of(xt * half + q * piece, piece)
        return u.at[zt, pl.ds(top, piece), :]

    def z_part(zt, m):
        return part(zt, 1 - x, 0) if m == U else part(zt, x, m)

    def ux_copy(zt, q):
        return remote(part(zt, x, q), part(zt, x, q), ux_ssem.at[zt, q], ux_rsem.at[zt, q], x_dev)

    def uu_copy(zt, m):
        return remote(z_part(zt, m), z_part(zt, m), uz_ssem.at[0, zt, m], uu_rsem.at[zt, m], up_dev)

    def ud_copy(zt, m):
        return remote(z_part(zt, m), z_part(zt, m), uz_ssem.at[1, zt, m], ud_rsem.at[zt, m], down_dev)

    def store(zt, xt, q):
        top = pl.multiple_of(xt * half + q * piece, piece)
        return pltpu.make_async_copy(
            part(zt, xt, q), update_hbm.at[zt, pl.ds(top, piece), :], u_out_sem.at[zt, xt, q]
        )

    def spread(m):
        @pl.when(has_above)
        def _():
            uu_copy(z, m).start()

        @pl.when(has_below)
        def _():
            ud_copy(z, m).start()

    for q in range(U):
        part(z, x, q)[...] = (precond[pl.ds(q * piece, piece), :] * scale).astype(bf16)
        ux_copy(z, q).start()
        spread(q)
        store(z, x, q).start()
    ux_copy(z, 0).wait_recv()
    spread(U)
    store(z, 1 - x, 0).start()

    window = pl.multiple_of(lax.div(i, 2) * cols, cols)
    turned = g[:, pl.ds(window, cols)].T
    columns[...] = jnp.where(lax.rem(i, 2) == 1, turned[span:, :], turned[:span, :])

    def grams(n, carry):
        r = pl.ds(pl.multiple_of(n * cols, cols), cols)
        left_gram = lax.dot_general(
            g[pl.ds(base, span), :], g[r, :], (((1,), (1,)), ((), ())), preferred_element_type=f32
        )
        stats[:, 0, r] = beta_stat * stats[:, 0, r] + (1.0 - beta_stat) * left_gram
        right_gram = jnp.dot(columns[...], g[:, r], preferred_element_type=f32)
        stats[:, 1, r] = beta_stat * stats[:, 1, r] + (1.0 - beta_stat) * right_gram
        return carry

    lax.fori_loop(0, width // cols, grams, 0)
    outs[2].start()

    def relay(zt, m, copy, onward):
        copy(zt, m).wait_recv()

        @pl.when(onward)
        def _():
            copy(zt, m).start()

        if 0 < m < U:
            ux_copy(zt, m).start()
        store(zt, 1 - x if m == U else x, 0 if m == U else m).start()

    for dist in range(1, Z):

        @pl.when(z - dist >= 0)
        def _(dist=dist):
            relay(z - dist, 0, uu_copy, has_above)

        @pl.when(z + dist < Z)
        def _(dist=dist):
            relay(z + dist, 0, ud_copy, has_below)

        for m in range(1, U + 1):

            @pl.when(z - dist >= 0)
            def _(dist=dist, m=m):
                relay(z - dist, m, uu_copy, has_above)

            @pl.when(z + dist < Z)
            def _(dist=dist, m=m):
                relay(z + dist, m, ud_copy, has_below)

    def arrive(zt):
        for q in range(1, U):
            ux_copy(zt, q).wait_recv()
            store(zt, 1 - x, q).start()

    arrive(z)
    for dist in range(1, Z):

        @pl.when(z - dist >= 0)
        def _(dist=dist):
            arrive(z - dist)

        @pl.when(z + dist < Z)
        def _(dist=dist):
            arrive(z + dist)

    l_y.wait_send()
    l_c.wait_send()
    l_f.wait_send()
    for tx in range(2):

        @pl.when(is_equal(x, tx) * at_home == 0)
        def _(tx=tx):
            r_copy(tx).wait_send()

    for k in range(1, 8):
        n_copy(k).wait_send()

    def sent(k, carry):
        for q in range(Q - 1):
            x_copy(k, q).wait_send()

        @pl.when(k < Z - 1)
        def _():
            for m in range(Q + 1):
                up_copy(k, m, k).wait_send()

        ux_last = is_equal(k, z)

        @pl.when(ux_last == 1)
        def _():
            ux_copy(k, 0).wait_send()

        for q in range(1, U):
            ux_copy(k, q).wait_send()
        for q in range(U):
            store(k, 0, q).wait()
            store(k, 1, q).wait()

        @pl.when((z >= k) & has_above)
        def _():
            for m in range(U + 1):
                uu_copy(k, m).wait_send()

        @pl.when((z <= k) & has_below)
        def _():
            for m in range(U + 1):
                ud_copy(k, m).wait_send()

        return carry

    lax.fori_loop(0, Z, sent, 0)
    for m in range(Q + 1):
        p_copy(m).wait_send()
    for rel in range(3):
        for cc in range(2 * Q):
            g_copy(rel, cc).wait_send()
    for out in outs:
        out.wait()


def finish_kernel(
    owner_ref, update_in, first_in, second_in, stats_in, update, first, second, stats, u, f, s, t, isem, osem
):
    Z, half = u.shape[0], u.shape[1] // 2
    moves = []
    for b in range(Z):
        for h in range(2):
            r = pl.ds(h * half, half)
            moves.append((update_in.at[owner_ref[b], r, :], u.at[b, r, :], update.at[b, r, :]))
    moves += [(first_in, f, first), (second_in, s, second), (stats_in, t, stats)]
    ins = [pltpu.make_async_copy(m[0], m[1], isem.at[n]) for n, m in enumerate(moves)]
    outs = [pltpu.make_async_copy(m[1], m[2], osem.at[n]) for n, m in enumerate(moves)]
    for copy in ins:
        copy.start()
    for copy, out in zip(ins, outs):
        copy.wait()
        out.start()
    for out in outs:
        out.wait()


def fused_body(
    activations,
    output_grads,
    owner,
    step_count,
    statistics,
    inverse_roots,
    first_moment,
    second_moment,
):
    f32, bf16 = jnp.float32, jnp.bfloat16
    tokens, width = activations.shape
    groups, cols = output_grads.shape[1:]
    span = statistics.shape[0]
    half, Q, U = width // 2, PARTS, PIECES
    rows = half // Q

    VMEM, DMA = pltpu.VMEM, pltpu.SemaphoreType.DMA
    hbm = pl.BlockSpec(memory_space=pl.ANY)
    smem = pl.BlockSpec(memory_space=pltpu.SMEM)
    results = (
        jax.ShapeDtypeStruct((groups, width, cols), bf16),
        jax.ShapeDtypeStruct((span, width), f32),
        jax.ShapeDtypeStruct((span, width), f32),
        jax.ShapeDtypeStruct((span, 2, width), f32),
    )
    params = dict(vmem_limit_bytes=60 * 1024 * 1024)
    update, first_new, second_new, new_stats = pl.pallas_call(
        functools.partial(step_kernel, groups),
        out_shape=results,
        in_specs=[smem, smem] + [hbm] * 6,
        out_specs=[hbm] * 4,
        scratch_shapes=[
            VMEM((tokens, width), bf16),
            VMEM((width, tokens), bf16),
            VMEM((groups, tokens, cols), bf16),
            VMEM((groups, Q, rows, cols), f32),
            VMEM((groups, rows, cols), f32),
            VMEM((groups, Q - 1, rows, cols), bf16),
            VMEM((groups, Q - 1, rows, cols), bf16),
            VMEM((groups, Q + 1, rows, cols), bf16),
            VMEM((groups, Q + 1, rows, cols), bf16),
            VMEM((groups, Q + 1, rows, cols), bf16),
            VMEM((Q + 1, rows, cols), bf16),
            VMEM((Q + 1, rows, cols), bf16),
            VMEM((width, width), bf16),
            VMEM((half, width), bf16),
            VMEM((2 * span, width), bf16),
            VMEM((span, width), bf16),
            VMEM((span, 2, width), bf16),
            VMEM((rows, cols), bf16),
            VMEM((rows, cols), bf16),
            VMEM((half, cols), f32),
            VMEM((span, width), f32),
            VMEM((span, width), f32),
            VMEM((span, width), bf16),
            VMEM((span, 2, width), f32),
            VMEM((groups, width, cols), bf16),
            VMEM((8, 8, cols), f32),
            DMA((6,)),
            DMA((3,)),
            DMA((groups, 2, U)),
            DMA((groups, Q - 1)),
            DMA((groups, Q - 1)),
            DMA((Q + 1,)),
            DMA((Q + 1,)),
            DMA((groups, Q + 1)),
            DMA((groups, Q + 1)),
            DMA((groups, Q + 1)),
            DMA((3, 2 * Q)),
            DMA((3, 2 * Q)),
            DMA((3,)),
            DMA((3,)),
            DMA((2,)),
            DMA((2,)),
            DMA((7,)),
            DMA((8,)),
            DMA((groups, U)),
            DMA((groups, U)),
            DMA((2, groups, U + 1)),
            DMA((groups, U + 1)),
            DMA((groups, U + 1)),
        ],
        compiler_params=pltpu.CompilerParams(collective_id=0, has_side_effects=True, **params),
        name="step_kernel",
    )(
        owner,
        step_count,
        activations,
        output_grads.transpose(1, 0, 2),
        inverse_roots,
        first_moment,
        second_moment,
        statistics,
    )
    moves = 2 * groups + 3
    update, first_new, second_new, new_stats = pl.pallas_call(
        finish_kernel,
        out_shape=results,
        in_specs=[smem] + [hbm] * 4,
        out_specs=[hbm] * 4,
        scratch_shapes=[VMEM(r.shape, r.dtype) for r in results] + [DMA((moves,)), DMA((moves,))],
        compiler_params=pltpu.CompilerParams(**params),
        name="finish_kernel",
    )(owner, update, first_new, second_new, new_stats)
    return (new_stats, first_new, second_new, update)


def dispatch(replicas, shards, *args):
    width, groups, cols = args[0].shape[1], args[1].shape[1], args[1].shape[2]
    whole = width % (256 * PARTS) == 0 and width % (256 * PIECES) == 0 and cols % 128 == 0
    if replicas == 2 * groups and shards == 4 and whole:
        return fused_body(*args)
    return body(*args)


def solution(mesh):
    placed = (
        P("replica", None),
        P("replica", None, "shard"),
        P(),
        P(),
        P(("replica", "shard"), None, None),
        P(("replica", "shard"), None, None),
        P(("replica", "shard"), None),
        P(("replica", "shard"), None),
    )
    return jax.shard_map(
        functools.partial(dispatch, mesh.shape["replica"], mesh.shape["shard"]),
        mesh=mesh,
        in_specs=placed,
        out_specs=(
            P(("replica", "shard"), None, None),
            P(("replica", "shard"), None),
            P(("replica", "shard"), None),
            P(None, None, "shard"),
        ),
        check_vma=False,
    )
```

```python
import functools

import jax
import jax.numpy as jnp
import numpy as np
from jax import lax
from jax.experimental import pallas as pl
from jax.experimental.pallas import tpu as pltpu
from jax.sharding import PartitionSpec as P

beta_stat = 0.9
beta_first = 0.9
beta_second = 0.999
eps_adam = 1e-08
eps_norm = 1e-06


def bits_of(extent):
    return extent.bit_length() - 1


def swap(value, axis, bit, keep=lambda i: True):
    n = lax.axis_size(axis)
    return lax.ppermute(value, axis, [(i, i ^ (1 << bit)) for i in range(n) if keep(i)])


def join(value, partner, axis, bit, dim):
    upper = (lax.axis_index(axis) >> bit) & 1 == 1
    return jnp.where(
        upper,
        jnp.concatenate([partner, value], dim),
        jnp.concatenate([value, partner], dim),
    )


def double(value, axis, bit, dim, keep=lambda i: True):
    return join(value, swap(value, axis, bit, keep), axis, bit, dim)


def reversed_bits(count):
    bits = bits_of(count)
    return [int(format(i, "b").zfill(bits)[::-1], 2) if bits else 0 for i in range(count)]


def reorder(value, count, dim):
    size = value.shape[dim] // count
    return jnp.concatenate(
        [lax.slice_in_dim(value, k * size, (k + 1) * size, axis=dim) for k in reversed_bits(count)],
        dim,
    )


def choose(values, picks, slot):
    out = values[picks[max(picks)]]
    for z in sorted(picks):
        if values[picks[z]] is not out:
            out = jnp.where(slot == z, values[picks[z]], out)
    return out


def body(
    activations,
    output_grads,
    owner,
    step_count,
    statistics,
    inverse_roots,
    first_moment,
    second_moment,
):
    f32, bf16 = jnp.float32, jnp.bfloat16
    width = activations.shape[1]
    groups = output_grads.shape[1]
    replicas = lax.axis_size("replica")
    shards = lax.axis_size("shard")
    size = replicas // groups
    local_bits = range(bits_of(size))
    shard_bits = list(range(bits_of(shards)))[::-1]
    span = statistics.shape[0]
    replica = lax.axis_index("replica")
    slot, local = replica // size, replica % size
    shard = lax.axis_index("shard")
    span_index = local * shards + shard

    slot_ids = jnp.arange(groups, dtype=jnp.int32)
    onehot = (owner[None, :] == slot_ids[:, None]).astype(jnp.int32)
    source = jnp.sum(onehot * slot_ids[None, :], axis=1)

    order = [sorted(range(groups), key=lambda s: (-abs(s - z), s)) for z in range(groups)]
    block_order = jnp.take(source, jnp.take(jnp.asarray(np.array(order, np.int32)), slot, axis=0))
    douts = output_grads.transpose(1, 0, 2)
    rounds = []
    for k in range(groups):
        part = lax.dot_general(
            activations,
            lax.dynamic_index_in_dim(douts, block_order[k], 0, keepdims=False),
            (((0,), (0,)), ((), ())),
            preferred_element_type=f32,
        )
        for bit in list(local_bits)[::-1]:
            half = part.shape[0] // 2
            mine = (local >> bit) & 1
            away = lax.dynamic_slice_in_dim(part, (1 - mine) * half, half, 0).astype(bf16)
            part = lax.dynamic_slice_in_dim(part, mine * half, half, 0) + swap(
                away, "replica", bit
            ).astype(f32)
        rounds.append(part)

    def shift(value, up, senders):
        step = size if up else -size
        return lax.ppermute(
            value,
            "replica",
            [(r, r + step) for r in range(replicas) if r // size in senders],
        )

    came_up = came_down = None
    for t in range(1, groups):
        ups = {z: order[z].index(groups - t + z) for z in range(t)}
        downs = {z: order[z].index(z + t - groups) for z in range(groups - t, groups)}
        up = choose(rounds, ups, slot)
        down = choose(rounds, downs, slot)
        if came_up is not None:
            up = up + came_up.astype(f32)
            down = down + came_down.astype(f32)
        came_up = shift(up.astype(bf16), True, ups)
        came_down = shift(down.astype(bf16), False, downs)
    own = (rounds[-1] + came_up.astype(f32) + came_down.astype(f32)).astype(bf16)

    rows = own.shape[0]
    top, low = own[: rows // 2], own[rows // 2 :]
    for bit in local_bits:
        top = double(top, "replica", bit, 0)
    for bit in shard_bits[:-1]:
        low = double(low, "shard", bit, 1)
        top = double(top, "shard", bit, 1)
    for bit in local_bits:
        low = double(low, "replica", bit, 0)
    for bit in shard_bits[-1:]:
        low = double(low, "shard", bit, 1)
        top = double(top, "shard", bit, 1)
    pieces = []
    for k in range(size):
        for half in (top, low):
            pieces.append(lax.slice_in_dim(half, k * (rows // 2), (k + 1) * (rows // 2), axis=0))
    full_grad = reorder(jnp.concatenate(pieces, 0), shards, 1)

    left_root = inverse_roots[:, 0, :]
    for bit in shard_bits:
        left_root = double(left_root, "shard", bit, 0)
    left_root = reorder(left_root, shards, 0)
    pairs = []
    for r in range(replicas):
        for s in range(shards):
            j = (r % size) * shards + s
            target = (r // size * size + j % size) * shards + j // size
            pairs.append((r * shards + s, target))
    right_root = lax.ppermute(inverse_roots[:, 1, :], ("replica", "shard"), pairs)
    for bit in local_bits:
        right_root = double(right_root, "replica", bit, 0)

    right_part = lax.dot_general(
        full_grad, right_root, (((1,), (1,)), ((), ())), preferred_element_type=f32
    )
    high = lax.reduce_precision(right_part, 8, 7)
    rest = right_part - high
    precond = jnp.dot(left_root, high.astype(bf16), preferred_element_type=f32) + jnp.dot(
        left_root, rest.astype(bf16), preferred_element_type=f32
    )

    rounded = lax.dynamic_slice_in_dim(full_grad, span_index * span, span, 0)
    exact = rounded.astype(f32)
    count_float = step_count[0].astype(f32)
    first_new = beta_first * first_moment + (1.0 - beta_first) * exact
    second_new = beta_second * second_moment + (1.0 - beta_second) * exact * exact
    first_hat = first_new / (1.0 - jnp.power(beta_first, count_float))
    second_hat = second_new / (1.0 - jnp.power(beta_second, count_float))
    adam_dir = first_hat / (jnp.sqrt(second_hat) + eps_adam)

    sums = jnp.stack([jnp.sum(adam_dir * adam_dir), jnp.sum(precond * precond)])
    sums = jnp.broadcast_to(sums[:, None], (2, 128))
    for bit in local_bits:
        sums = sums + swap(sums, "replica", bit)
    for bit in shard_bits:
        sums = sums + swap(sums, "shard", bit)
    scale = jnp.sqrt(sums[0, 0]) / (jnp.sqrt(sums[1, 0]) + eps_norm)
    grafted = (precond * scale).astype(bf16)

    def complete(value, zs):
        for bit in local_bits:
            value = double(value, "replica", bit, 0, lambda r: r // size in zs)
        return value

    whole = {0: complete(grafted, range(groups))}
    up = down = grafted
    ups, downs = {}, {}
    for t in range(1, groups):
        up = shift(up, True, range(t - 1, groups - 1))
        down = shift(down, False, range(1, groups - t + 1))
        ups[t] = complete(up, range(t, groups))
        downs[t] = complete(down, range(0, groups - t))
    for m in range(1, groups):
        whole[m] = jnp.where(slot + m < groups, downs[m], ups[groups - m])
    update = jnp.zeros((groups,) + whole[0].shape, bf16)
    for m in range(groups):
        block = jnp.take(source, (slot + m) % groups)
        update = lax.dynamic_update_index_in_dim(update, whole[m], block, 0)

    grad_columns = lax.dynamic_slice_in_dim(full_grad, span_index * span, span, 1)
    left_gram = lax.dot_general(
        rounded, full_grad, (((1,), (1,)), ((), ())), preferred_element_type=f32
    )
    right_gram = lax.dot_general(
        grad_columns, full_grad, (((0,), (0,)), ((), ())), preferred_element_type=f32
    )
    new_left = beta_stat * statistics[:, 0, :] + (1.0 - beta_stat) * left_gram
    new_right = beta_stat * statistics[:, 1, :] + (1.0 - beta_stat) * right_gram
    new_stats = jnp.stack([new_left, new_right], axis=1)
    return (new_stats, first_new, second_new, update)


PARTS = 3
PIECES = 6


def is_equal(a, b):
    return lax.div(jnp.int32(1), 1 + (a - b) * (a - b))


def block_orders(groups):
    return [sorted(range(groups), key=lambda s: (-abs(s - z), s)) for z in range(groups)]


def power(base, count):
    out = jnp.float32(1.0)
    for bit in range(16):
        odd = lax.rem(lax.div(count, jnp.int32(1 << bit)), jnp.int32(2)) == 1
        out = out * jnp.where(odd, jnp.float32(base ** (1 << bit)), jnp.float32(1.0))
    return out


def step_kernel(
    groups,
    owner_ref,
    count_ref,
    a,
    d,
    roots_hbm,
    first_hbm,
    second_hbm,
    stats_hbm,
    u,
    first,
    second,
    stats,
    at,
    acc,
    away0,
    x_send,
    x_recv,
    z_send,
    up_recv,
    down_recv,
    p_send,
    p_recv,
    g,
    left,
    right,
    stage,
    roots,
    high,
    low,
    precond,
    columns,
    norms,
    load_sem,
    x_ssem,
    x_rsem,
    p_ssem,
    p_rsem,
    z_ssem,
    up_rsem,
    down_rsem,
    g_ssem,
    g_rsem,
    l_ssem,
    l_rsem,
    r_ssem,
    r_rsem,
    n_ssem,
    n_rsem,
    ux_ssem,
    ux_rsem,
    uz_ssem,
    uu_rsem,
    ud_rsem,
):
    f32, bf16 = jnp.float32, jnp.bfloat16
    Z, Q, U = groups, PARTS, PIECES
    own = Z - 1
    width = g.shape[0]
    half = width // 2
    rows = half // Q
    cols = d.shape[2]
    span = first.shape[0]
    replica, s = lax.axis_index("replica"), lax.axis_index("shard")
    z, x = lax.div(replica, 2), lax.rem(replica, 2)
    y, c = lax.div(s, 2), lax.rem(s, 2)
    i = x * 4 + s
    x_dev = (z * 2 + 1 - x, s)
    y_dev = (replica, (1 - y) * 2 + c)
    c_dev = (replica, y * 2 + 1 - c)
    up_dev = (replica + 2, s)
    down_dev = (replica - 2, s)

    def remote(src, dst, ssem, rsem, dev):
        return pltpu.make_async_remote_copy(
            src_ref=src,
            dst_ref=dst,
            send_sem=ssem,
            recv_sem=rsem,
            device_id=dev,
            device_id_type=pl.DeviceIdType.MESH,
        )

    def peer(k):
        j = lax.rem(i + k, 8)
        return (z * 2 + lax.div(j, 4), lax.rem(j, 4))

    loads = [
        pltpu.make_async_copy(roots_hbm, roots, load_sem.at[0]),
        pltpu.make_async_copy(first_hbm, first, load_sem.at[1]),
        pltpu.make_async_copy(second_hbm, second, load_sem.at[2]),
        pltpu.make_async_copy(stats_hbm, stats, load_sem.at[3]),
    ]

    barrier = pltpu.get_barrier_semaphore()

    def greet(dev):
        pl.semaphore_signal(barrier, inc=1, device_id=dev, device_id_type=pl.DeviceIdType.MESH)

    for k in range(1, 8):
        greet(peer(k))
    has_below, has_above = z > 0, z < Z - 1

    @pl.when(has_above)
    def _():
        greet(up_dev)

    @pl.when(has_below)
    def _():
        greet(down_dev)

    for load in loads:
        load.start()
    orders = block_orders(Z)

    def target(k):
        return sum(
            is_equal(z, p) * is_equal(k, q) * orders[p][q] for p in range(Z) for q in range(Z)
        )

    def x_copy(k, q):
        return remote(x_send.at[k, q], x_recv.at[k, q], x_ssem.at[k, q], x_rsem.at[k, q], x_dev)

    def up_copy(k, m, t):
        return remote(z_send.at[k, m], up_recv.at[t, m], z_ssem.at[k, m], up_rsem.at[t, m], up_dev)

    def down_copy(k, m, t):
        return remote(
            z_send.at[k, m], down_recv.at[t, m], z_ssem.at[k, m], down_rsem.at[t, m], down_dev
        )

    def awaited(t):
        return (t > z) & has_below, (t < z) & has_above

    def gather(ref, k, m, t, from_below, from_above):
        @pl.when(from_below)
        def _():
            up_copy(k, m, t).wait_recv()
            ref[...] = ref[...] + up_recv[t, m].astype(f32)

        @pl.when(from_above)
        def _():
            down_copy(k, m, t).wait_recv()
            ref[...] = ref[...] + down_recv[t, m].astype(f32)

    def pass_on(ref, k, m):
        t = target(k)
        gather(ref, k, m, t, *awaited(t))
        z_send[k, m] = ref[...].astype(bf16)

        @pl.when(t > z)
        def _():
            up_copy(k, m, t).start()

        @pl.when(t < z)
        def _():
            down_copy(k, m, t).start()

    def left_rows(shard):
        return left.at[pl.ds(pl.multiple_of(shard * span, span), span)]

    place = right.at[pl.ds(pl.multiple_of(c * span, span), span)]
    at_home = is_equal(x, y) * is_equal(y, c)
    s_y = (1 - y) * 2 + c
    l_y = remote(left_rows(s), left_rows(s), l_ssem.at[0], l_rsem.at[0], y_dev)
    l_c = remote(left_rows(s), left_rows(s), l_ssem.at[1], l_rsem.at[1], c_dev)
    l_f = remote(left_rows(s_y), left_rows(s_y), l_ssem.at[2], l_rsem.at[2], c_dev)

    def r_copy(tx):
        return remote(stage, place, r_ssem.at[tx], r_rsem.at[c], (z * 2 + tx, x * 2 + y))

    def send_roots():
        loads[0].wait()
        stage[...] = roots[:, 1, :]
        for tx in range(2):

            @pl.when(is_equal(x, tx) * at_home == 0)
            def _(tx=tx):
                r_copy(tx).start()

        left_rows(s)[...] = roots[:, 0, :]
        l_y.start()
        l_c.start()

        @pl.when(at_home == 1)
        def _():
            place[...] = stage[...]

    def multiply(k, carry):
        t = target(k)
        block = jnp.int32(0)
        for b in range(Z):
            block = jnp.where(owner_ref[b] == t, jnp.int32(b), block)

        def product(side, q):
            r = pl.ds(pl.multiple_of(side * half + q * rows, rows), rows)

            @pl.when(k == 0)
            def _():
                at[r, :] = a[:, r].T

            return jnp.dot(at[r, :], d[block], preferred_element_type=f32)

        def send_away(q, carry):
            x_send[k, q - 1] = product(1 - x, q).astype(bf16)

            @pl.when(k < own - 1)
            def _():
                x_copy(k, q - 1).start()

            return carry

        def keep(q, carry):
            acc[k, q] = product(x, q)
            return carry

        from_below, from_above = awaited(t)
        waits = from_below | from_above

        def pass_first():
            pass_on(acc.at[k, 0], k, 0)
            pass_on(away0.at[k], k, Q)

        send_away(1, 0)
        keep(0, 0)
        away0[k] = product(1 - x, 0)

        @pl.when((k < own) & jnp.logical_not(waits))
        def _():
            pass_first()

        lax.fori_loop(2, Q, send_away, 0)
        lax.fori_loop(1, Q, keep, 0)

        @pl.when(k == 0)
        def _():
            send_roots()

        @pl.when((k < own) & waits)
        def _():
            pass_first()

        return carry

    pl.semaphore_wait(barrier, 9 - is_equal(z, 0) - is_equal(z, Z - 1))
    lax.fori_loop(0, Z, multiply, 0)

    def pass_reduced(n, carry):
        k, q = lax.div(n, Q - 1), lax.rem(n, Q - 1)
        x_copy(k, q).wait_recv()
        acc[k, q + 1] = acc[k, q + 1] + x_recv[k, q].astype(f32)
        pass_on(acc.at[k, q + 1], k, q + 1)
        return carry

    def p_copy(m):
        return remote(p_send.at[m], p_recv.at[m], p_ssem.at[m], p_rsem.at[m], x_dev)

    def own_sum(m):
        ref = away0.at[own] if m == Q else acc.at[own, m]
        gather(ref, own, m, z, has_below, has_above)
        p_send[m] = ref[...].astype(bf16)
        p_copy(m).start()

    def own_first():
        own_sum(0)
        own_sum(Q)
        for k in (own - 1, own):
            for q in range(Q - 1):
                x_copy(k, q).start()

    @pl.when(has_below & has_above)
    def _():
        own_first()

    lax.fori_loop(0, (own - 1) * (Q - 1), pass_reduced, 0)
    l_y.wait_recv()
    l_f.start()

    @pl.when(jnp.logical_not(has_below & has_above))
    def _():
        own_first()

    def tile(cc, shard):
        top = pl.multiple_of(cc * rows, rows)
        side = pl.multiple_of(shard * cols, cols)
        return g.at[pl.ds(top, rows), pl.ds(side, cols)]

    def g_copy(rel, cc):
        ref = tile(cc, s_y if rel == 2 else s)
        dev = y_dev if rel == 1 else c_dev
        return remote(ref, ref, g_ssem.at[rel, cc], g_rsem.at[rel, cc], dev)

    plan = [(0, 0), (1, 0)] + [(0, q) for q in range(1, Q)] + [(1, q) for q in range(1, Q)]

    def chunk(j):
        side, q = plan[j]
        return (x if side == 0 else 1 - x) * Q + q

    def put(j):
        side, q = plan[j]
        if side == 0 and q > 0:
            own_sum(q)
            x_copy(own, q - 1).wait_recv()
            value = acc[own, q] + x_recv[own, q - 1].astype(f32)
        elif side == 0:
            p_copy(Q).wait_recv()
            value = acc[own, 0] + p_recv[Q].astype(f32)
        elif q == 0:
            p_copy(0).wait_recv()
            value = away0[own] + p_recv[0].astype(f32)
        else:
            p_copy(q).wait_recv()
            value = x_send[own, q - 1].astype(f32) + p_recv[q].astype(f32)
        cc = chunk(j)
        tile(cc, s)[...] = value.astype(bf16)
        g_copy(1, cc).start()
        g_copy(0, cc).start()

    def forward(j):
        g_copy(1, chunk(j)).wait_recv()
        g_copy(2, chunk(j)).start()

    def precondition(j):
        cc = chunk(j)
        g_copy(0, cc).wait_recv()
        g_copy(2, cc).wait_recv()
        r = pl.ds(pl.multiple_of(cc * rows, rows), rows)
        value = lax.dot_general(
            g[r, :], right[...], (((1,), (1,)), ((), ())), preferred_element_type=f32
        )
        top = value.astype(bf16)
        high[...] = top
        low[...] = (value - top.astype(f32)).astype(bf16)

        def times_left(n, carry):
            o = pl.ds(pl.multiple_of(n * rows, rows), rows)
            value = jnp.dot(left[o, r], high[...], preferred_element_type=f32) + jnp.dot(
                left[o, r], low[...], preferred_element_type=f32
            )
            precond[o, :] = value if j == 0 else precond[o, :] + value
            return carry

        lax.fori_loop(0, Q, times_left, 0)

    base = pl.multiple_of(i * span, span)
    lot = 16

    def adam(n, carry):
        total, first_bias, second_bias = carry
        r = pl.ds(pl.multiple_of(n * lot, lot), lot)
        grad = g[pl.ds(pl.multiple_of(base + n * lot, lot), lot), :].astype(f32)
        first_new = beta_first * first[r, :] + (1.0 - beta_first) * grad
        second_new = beta_second * second[r, :] + (1.0 - beta_second) * grad * grad
        first[r, :] = first_new
        second[r, :] = second_new
        value = (first_new * first_bias) / (jnp.sqrt(second_new * second_bias) + eps_adam)
        return total + value * value, first_bias, second_bias

    def roots_here():
        for rc in range(2):

            @pl.when(at_home * is_equal(c, rc) == 0)
            def _(rc=rc):
                remote(
                    stage, right.at[pl.ds(rc * span, span)], r_ssem.at[0], r_rsem.at[rc], x_dev
                ).wait_recv()

        l_c.wait_recv()
        l_f.wait_recv()

    def adam_sum():
        for load in loads[1:]:
            load.wait()
        first_bias = 1.0 / jnp.full((1, width), 1.0 - power(beta_first, count_ref[0]))
        second_bias = 1.0 / jnp.full((1, width), 1.0 - power(beta_second, count_ref[0]))
        total, _, _ = lax.fori_loop(
            0, span // lot, adam, (jnp.zeros((lot, width), f32), first_bias, second_bias)
        )
        return jnp.sum(total)

    last = len(plan)
    for j in range(last):
        if j == 2:
            lax.fori_loop((own - 1) * (Q - 1), own * (Q - 1), pass_reduced, 0)
        put(j)
        if j >= 2:
            forward(j - 2)
        if j == 3:
            roots_here()
        if j >= 3:
            precondition(j - 3)
    forward(last - 2)
    precondition(last - 3)
    precondition(last - 2)
    forward(last - 1)
    adam_squares = adam_sum()
    precondition(last - 1)

    def squares(n, total):
        value = precond[pl.ds(pl.multiple_of(n * lot, lot), lot), :]
        return total + value * value

    precond_squares = jnp.sum(
        lax.fori_loop(0, half // lot, squares, jnp.zeros((lot, cols), f32))
    )
    which = lax.broadcasted_iota(jnp.int32, norms.shape[1:], 0)
    norms[i] = jnp.where(which == 0, adam_squares, precond_squares)

    def n_copy(k):
        return remote(norms.at[i], norms.at[i], n_ssem.at[k - 1], n_rsem.at[i], peer(k))

    for k in range(1, 8):
        n_copy(k).start()
    for k in range(1, 8):
        j = lax.rem(i + k, 8)
        remote(norms.at[j], norms.at[j], n_ssem.at[k - 1], n_rsem.at[j], peer(k)).wait_recv()
    total = norms[0]
    for k in range(1, 8):
        total = total + norms[k]
    scale = jnp.sqrt(total[0:1, :]) / (jnp.sqrt(total[1:2, :]) + eps_norm)

    piece = half // U

    def part(zt, xt, q):
        top = pl.multiple_of(xt * half + q * piece, piece)
        return u.at[zt, pl.ds(top, piece), :]

    def z_part(zt, m):
        return part(zt, 1 - x, 0) if m == U else part(zt, x, m)

    def ux_copy(zt, q):
        return remote(part(zt, x, q), part(zt, x, q), ux_ssem.at[zt, q], ux_rsem.at[zt, q], x_dev)

    def uu_copy(zt, m):
        return remote(z_part(zt, m), z_part(zt, m), uz_ssem.at[0, zt, m], uu_rsem.at[zt, m], up_dev)

    def ud_copy(zt, m):
        return remote(z_part(zt, m), z_part(zt, m), uz_ssem.at[1, zt, m], ud_rsem.at[zt, m], down_dev)

    def spread(m):
        @pl.when(has_above)
        def _():
            uu_copy(z, m).start()

        @pl.when(has_below)
        def _():
            ud_copy(z, m).start()

    for q in range(U):
        part(z, x, q)[...] = (precond[pl.ds(q * piece, piece), :] * scale).astype(bf16)
        ux_copy(z, q).start()
        spread(q)
    ux_copy(z, 0).wait_recv()
    spread(U)

    window = pl.multiple_of(lax.div(i, 2) * cols, cols)
    turned = g[:, pl.ds(window, cols)].T
    columns[...] = jnp.where(lax.rem(i, 2) == 1, turned[span:, :], turned[:span, :])

    def grams(n, carry):
        r = pl.ds(pl.multiple_of(n * cols, cols), cols)
        left_gram = lax.dot_general(
            g[pl.ds(base, span), :], g[r, :], (((1,), (1,)), ((), ())), preferred_element_type=f32
        )
        stats[:, 0, r] = beta_stat * stats[:, 0, r] + (1.0 - beta_stat) * left_gram
        right_gram = jnp.dot(columns[...], g[:, r], preferred_element_type=f32)
        stats[:, 1, r] = beta_stat * stats[:, 1, r] + (1.0 - beta_stat) * right_gram
        return carry

    lax.fori_loop(0, width // cols, grams, 0)

    def relay(zt, m, copy, onward):
        copy(zt, m).wait_recv()

        @pl.when(onward)
        def _():
            copy(zt, m).start()

        if 0 < m < U:
            ux_copy(zt, m).start()

    for dist in range(1, Z):

        @pl.when(z - dist >= 0)
        def _(dist=dist):
            relay(z - dist, 0, uu_copy, has_above)

        @pl.when(z + dist < Z)
        def _(dist=dist):
            relay(z + dist, 0, ud_copy, has_below)

        for m in range(1, U + 1):

            @pl.when(z - dist >= 0)
            def _(dist=dist, m=m):
                relay(z - dist, m, uu_copy, has_above)

            @pl.when(z + dist < Z)
            def _(dist=dist, m=m):
                relay(z + dist, m, ud_copy, has_below)

    def arrive(zt):
        for q in range(1, U):
            ux_copy(zt, q).wait_recv()

    arrive(z)
    for dist in range(1, Z):

        @pl.when(z - dist >= 0)
        def _(dist=dist):
            arrive(z - dist)

        @pl.when(z + dist < Z)
        def _(dist=dist):
            arrive(z + dist)

    l_y.wait_send()
    l_c.wait_send()
    l_f.wait_send()
    for tx in range(2):

        @pl.when(is_equal(x, tx) * at_home == 0)
        def _(tx=tx):
            r_copy(tx).wait_send()

    for k in range(1, 8):
        n_copy(k).wait_send()

    def sent(k, carry):
        for q in range(Q - 1):
            x_copy(k, q).wait_send()

        @pl.when(k < Z - 1)
        def _():
            for m in range(Q + 1):
                up_copy(k, m, k).wait_send()

        ux_last = is_equal(k, z)

        @pl.when(ux_last == 1)
        def _():
            ux_copy(k, 0).wait_send()

        for q in range(1, U):
            ux_copy(k, q).wait_send()

        @pl.when((z >= k) & has_above)
        def _():
            for m in range(U + 1):
                uu_copy(k, m).wait_send()

        @pl.when((z <= k) & has_below)
        def _():
            for m in range(U + 1):
                ud_copy(k, m).wait_send()

        return carry

    lax.fori_loop(0, Z, sent, 0)
    for m in range(Q + 1):
        p_copy(m).wait_send()
    for rel in range(3):
        for cc in range(2 * Q):
            g_copy(rel, cc).wait_send()


def finish_kernel(owner_ref, u, first, second, stats, update, first_out, second_out, stats_out, sems):
    copies = [
        pltpu.make_async_copy(u.at[owner_ref[b]], update.at[b], sems.at[b])
        for b in range(u.shape[0])
    ]
    for ref, out in ((stats, stats_out), (first, first_out), (second, second_out)):
        copies.append(pltpu.make_async_copy(ref, out, sems.at[len(copies)]))
    for copy in copies:
        copy.start()
    for copy in copies:
        copy.wait()


def fused_body(
    activations,
    output_grads,
    owner,
    step_count,
    statistics,
    inverse_roots,
    first_moment,
    second_moment,
):
    f32, bf16 = jnp.float32, jnp.bfloat16
    tokens, width = activations.shape
    groups, cols = output_grads.shape[1:]
    span = statistics.shape[0]
    half, Q, U = width // 2, PARTS, PIECES
    rows = half // Q

    VMEM, DMA = pltpu.VMEM, pltpu.SemaphoreType.DMA
    hbm = pl.BlockSpec(memory_space=pl.ANY)
    smem = pl.BlockSpec(memory_space=pltpu.SMEM)
    results = (
        jax.ShapeDtypeStruct((groups, width, cols), bf16),
        jax.ShapeDtypeStruct((span, width), f32),
        jax.ShapeDtypeStruct((span, width), f32),
        jax.ShapeDtypeStruct((span, 2, width), f32),
    )
    vmem = pl.BlockSpec(memory_space=pltpu.VMEM)
    update, first_new, second_new, new_stats = pl.pallas_call(
        functools.partial(step_kernel, groups),
        out_shape=tuple(VMEM(r.shape, r.dtype) for r in results),
        in_specs=[smem, smem, vmem, vmem] + [hbm] * 4,
        out_specs=[vmem] * 4,
        scratch_shapes=[
            VMEM((width, tokens), bf16),
            VMEM((groups, Q, rows, cols), f32),
            VMEM((groups, rows, cols), f32),
            VMEM((groups, Q - 1, rows, cols), bf16),
            VMEM((groups, Q - 1, rows, cols), bf16),
            VMEM((groups, Q + 1, rows, cols), bf16),
            VMEM((groups, Q + 1, rows, cols), bf16),
            VMEM((groups, Q + 1, rows, cols), bf16),
            VMEM((Q + 1, rows, cols), bf16),
            VMEM((Q + 1, rows, cols), bf16),
            VMEM((width, width), bf16),
            VMEM((half, width), bf16),
            VMEM((2 * span, width), bf16),
            VMEM((span, width), bf16),
            VMEM((span, 2, width), bf16),
            VMEM((rows, cols), bf16),
            VMEM((rows, cols), bf16),
            VMEM((half, cols), f32),
            VMEM((span, width), bf16),
            VMEM((8, 8, cols), f32),
            DMA((4,)),
            DMA((groups, Q - 1)),
            DMA((groups, Q - 1)),
            DMA((Q + 1,)),
            DMA((Q + 1,)),
            DMA((groups, Q + 1)),
            DMA((groups, Q + 1)),
            DMA((groups, Q + 1)),
            DMA((3, 2 * Q)),
            DMA((3, 2 * Q)),
            DMA((3,)),
            DMA((3,)),
            DMA((2,)),
            DMA((2,)),
            DMA((7,)),
            DMA((8,)),
            DMA((groups, U)),
            DMA((groups, U)),
            DMA((2, groups, U + 1)),
            DMA((groups, U + 1)),
            DMA((groups, U + 1)),
        ],
        compiler_params=pltpu.CompilerParams(
            collective_id=0, has_side_effects=True, vmem_limit_bytes=44 * 1024 * 1024
        ),
        name="step_kernel",
    )(
        owner,
        step_count,
        pltpu.with_memory_space_constraint(activations, pltpu.VMEM),
        pltpu.with_memory_space_constraint(output_grads.transpose(1, 0, 2), pltpu.VMEM),
        inverse_roots,
        first_moment,
        second_moment,
        statistics,
    )
    update, first_new, second_new, new_stats = pl.pallas_call(
        finish_kernel,
        out_shape=results,
        in_specs=[smem] + [vmem] * 4,
        out_specs=[hbm] * 4,
        scratch_shapes=[DMA((groups + 3,))],
        compiler_params=pltpu.CompilerParams(vmem_limit_bytes=16 * 1024 * 1024),
        name="finish_kernel",
    )(owner, update, first_new, second_new, new_stats)
    return (new_stats, first_new, second_new, update)


def dispatch(replicas, shards, *args):
    width, groups, cols = args[0].shape[1], args[1].shape[1], args[1].shape[2]
    whole = width % (256 * PARTS) == 0 and width % (256 * PIECES) == 0 and cols % 128 == 0
    if replicas == 2 * groups and shards == 4 and whole:
        return fused_body(*args)
    return body(*args)


def solution(mesh):
    placed = (
        P("replica", None),
        P("replica", None, "shard"),
        P(),
        P(),
        P(("replica", "shard"), None, None),
        P(("replica", "shard"), None, None),
        P(("replica", "shard"), None),
        P(("replica", "shard"), None),
    )
    return jax.shard_map(
        functools.partial(dispatch, mesh.shape["replica"], mesh.shape["shard"]),
        mesh=mesh,
        in_specs=placed,
        out_specs=(
            P(("replica", "shard"), None, None),
            P(("replica", "shard"), None),
            P(("replica", "shard"), None),
            P(None, None, "shard"),
        ),
        check_vma=False,
    )
```

```python
import functools

import jax
import jax.numpy as jnp
import numpy as np
from jax import lax
from jax.experimental import pallas as pl
from jax.experimental.pallas import tpu as pltpu
from jax.sharding import PartitionSpec as P

beta_stat = 0.9
beta_first = 0.9
beta_second = 0.999
eps_adam = 1e-08
eps_norm = 1e-06


def bits_of(extent):
    return extent.bit_length() - 1


def swap(value, axis, bit, keep=lambda i: True):
    n = lax.axis_size(axis)
    return lax.ppermute(value, axis, [(i, i ^ (1 << bit)) for i in range(n) if keep(i)])


def join(value, partner, axis, bit, dim):
    upper = (lax.axis_index(axis) >> bit) & 1 == 1
    return jnp.where(
        upper,
        jnp.concatenate([partner, value], dim),
        jnp.concatenate([value, partner], dim),
    )


def double(value, axis, bit, dim, keep=lambda i: True):
    return join(value, swap(value, axis, bit, keep), axis, bit, dim)


def reversed_bits(count):
    bits = bits_of(count)
    return [int(format(i, "b").zfill(bits)[::-1], 2) if bits else 0 for i in range(count)]


def reorder(value, count, dim):
    size = value.shape[dim] // count
    return jnp.concatenate(
        [lax.slice_in_dim(value, k * size, (k + 1) * size, axis=dim) for k in reversed_bits(count)],
        dim,
    )


def choose(values, picks, slot):
    out = values[picks[max(picks)]]
    for z in sorted(picks):
        if values[picks[z]] is not out:
            out = jnp.where(slot == z, values[picks[z]], out)
    return out


def body(
    activations,
    output_grads,
    owner,
    step_count,
    statistics,
    inverse_roots,
    first_moment,
    second_moment,
):
    f32, bf16 = jnp.float32, jnp.bfloat16
    width = activations.shape[1]
    groups = output_grads.shape[1]
    replicas = lax.axis_size("replica")
    shards = lax.axis_size("shard")
    size = replicas // groups
    local_bits = range(bits_of(size))
    shard_bits = list(range(bits_of(shards)))[::-1]
    span = statistics.shape[0]
    replica = lax.axis_index("replica")
    slot, local = replica // size, replica % size
    shard = lax.axis_index("shard")
    span_index = local * shards + shard

    slot_ids = jnp.arange(groups, dtype=jnp.int32)
    onehot = (owner[None, :] == slot_ids[:, None]).astype(jnp.int32)
    source = jnp.sum(onehot * slot_ids[None, :], axis=1)

    order = [sorted(range(groups), key=lambda s: (-abs(s - z), s)) for z in range(groups)]
    block_order = jnp.take(source, jnp.take(jnp.asarray(np.array(order, np.int32)), slot, axis=0))
    douts = output_grads.transpose(1, 0, 2)
    rounds = []
    for k in range(groups):
        part = lax.dot_general(
            activations,
            lax.dynamic_index_in_dim(douts, block_order[k], 0, keepdims=False),
            (((0,), (0,)), ((), ())),
            preferred_element_type=f32,
        )
        for bit in list(local_bits)[::-1]:
            half = part.shape[0] // 2
            mine = (local >> bit) & 1
            away = lax.dynamic_slice_in_dim(part, (1 - mine) * half, half, 0).astype(bf16)
            part = lax.dynamic_slice_in_dim(part, mine * half, half, 0) + swap(
                away, "replica", bit
            ).astype(f32)
        rounds.append(part)

    def shift(value, up, senders):
        step = size if up else -size
        return lax.ppermute(
            value,
            "replica",
            [(r, r + step) for r in range(replicas) if r // size in senders],
        )

    came_up = came_down = None
    for t in range(1, groups):
        ups = {z: order[z].index(groups - t + z) for z in range(t)}
        downs = {z: order[z].index(z + t - groups) for z in range(groups - t, groups)}
        up = choose(rounds, ups, slot)
        down = choose(rounds, downs, slot)
        if came_up is not None:
            up = up + came_up.astype(f32)
            down = down + came_down.astype(f32)
        came_up = shift(up.astype(bf16), True, ups)
        came_down = shift(down.astype(bf16), False, downs)
    own = (rounds[-1] + came_up.astype(f32) + came_down.astype(f32)).astype(bf16)

    rows = own.shape[0]
    top, low = own[: rows // 2], own[rows // 2 :]
    for bit in local_bits:
        top = double(top, "replica", bit, 0)
    for bit in shard_bits[:-1]:
        low = double(low, "shard", bit, 1)
        top = double(top, "shard", bit, 1)
    for bit in local_bits:
        low = double(low, "replica", bit, 0)
    for bit in shard_bits[-1:]:
        low = double(low, "shard", bit, 1)
        top = double(top, "shard", bit, 1)
    pieces = []
    for k in range(size):
        for half in (top, low):
            pieces.append(lax.slice_in_dim(half, k * (rows // 2), (k + 1) * (rows // 2), axis=0))
    full_grad = reorder(jnp.concatenate(pieces, 0), shards, 1)

    left_root = inverse_roots[:, 0, :]
    for bit in shard_bits:
        left_root = double(left_root, "shard", bit, 0)
    left_root = reorder(left_root, shards, 0)
    pairs = []
    for r in range(replicas):
        for s in range(shards):
            j = (r % size) * shards + s
            target = (r // size * size + j % size) * shards + j // size
            pairs.append((r * shards + s, target))
    right_root = lax.ppermute(inverse_roots[:, 1, :], ("replica", "shard"), pairs)
    for bit in local_bits:
        right_root = double(right_root, "replica", bit, 0)

    right_part = lax.dot_general(
        full_grad, right_root, (((1,), (1,)), ((), ())), preferred_element_type=f32
    )
    high = lax.reduce_precision(right_part, 8, 7)
    rest = right_part - high
    precond = jnp.dot(left_root, high.astype(bf16), preferred_element_type=f32) + jnp.dot(
        left_root, rest.astype(bf16), preferred_element_type=f32
    )

    rounded = lax.dynamic_slice_in_dim(full_grad, span_index * span, span, 0)
    exact = rounded.astype(f32)
    count_float = step_count[0].astype(f32)
    first_new = beta_first * first_moment + (1.0 - beta_first) * exact
    second_new = beta_second * second_moment + (1.0 - beta_second) * exact * exact
    first_hat = first_new / (1.0 - jnp.power(beta_first, count_float))
    second_hat = second_new / (1.0 - jnp.power(beta_second, count_float))
    adam_dir = first_hat / (jnp.sqrt(second_hat) + eps_adam)

    sums = jnp.stack([jnp.sum(adam_dir * adam_dir), jnp.sum(precond * precond)])
    sums = jnp.broadcast_to(sums[:, None], (2, 128))
    for bit in local_bits:
        sums = sums + swap(sums, "replica", bit)
    for bit in shard_bits:
        sums = sums + swap(sums, "shard", bit)
    scale = jnp.sqrt(sums[0, 0]) / (jnp.sqrt(sums[1, 0]) + eps_norm)
    grafted = (precond * scale).astype(bf16)

    def complete(value, zs):
        for bit in local_bits:
            value = double(value, "replica", bit, 0, lambda r: r // size in zs)
        return value

    whole = {0: complete(grafted, range(groups))}
    up = down = grafted
    ups, downs = {}, {}
    for t in range(1, groups):
        up = shift(up, True, range(t - 1, groups - 1))
        down = shift(down, False, range(1, groups - t + 1))
        ups[t] = complete(up, range(t, groups))
        downs[t] = complete(down, range(0, groups - t))
    for m in range(1, groups):
        whole[m] = jnp.where(slot + m < groups, downs[m], ups[groups - m])
    update = jnp.zeros((groups,) + whole[0].shape, bf16)
    for m in range(groups):
        block = jnp.take(source, (slot + m) % groups)
        update = lax.dynamic_update_index_in_dim(update, whole[m], block, 0)

    grad_columns = lax.dynamic_slice_in_dim(full_grad, span_index * span, span, 1)
    left_gram = lax.dot_general(
        rounded, full_grad, (((1,), (1,)), ((), ())), preferred_element_type=f32
    )
    right_gram = lax.dot_general(
        grad_columns, full_grad, (((0,), (0,)), ((), ())), preferred_element_type=f32
    )
    new_left = beta_stat * statistics[:, 0, :] + (1.0 - beta_stat) * left_gram
    new_right = beta_stat * statistics[:, 1, :] + (1.0 - beta_stat) * right_gram
    new_stats = jnp.stack([new_left, new_right], axis=1)
    return (new_stats, first_new, second_new, update)


PARTS = 3
PIECES = 6


def is_equal(a, b):
    return lax.div(jnp.int32(1), 1 + (a - b) * (a - b))


def block_orders(groups):
    return [sorted(range(groups), key=lambda s: (-abs(s - z), s)) for z in range(groups)]


def power(base, count):
    out = jnp.float32(1.0)
    for bit in range(16):
        odd = lax.rem(lax.div(count, jnp.int32(1 << bit)), jnp.int32(2)) == 1
        out = out * jnp.where(odd, jnp.float32(base ** (1 << bit)), jnp.float32(1.0))
    return out


def step_kernel(
    groups,
    owner_ref,
    count_ref,
    a,
    d,
    roots_hbm,
    first_hbm,
    second_hbm,
    stats_hbm,
    u,
    first,
    second,
    stats,
    at,
    acc,
    away0,
    x_send,
    x_recv,
    z_send,
    up_recv,
    down_recv,
    p_send,
    p_recv,
    g,
    left,
    right,
    stage,
    roots,
    high,
    low,
    precond,
    columns,
    norms,
    load_sem,
    x_ssem,
    x_rsem,
    p_ssem,
    p_rsem,
    z_ssem,
    up_rsem,
    down_rsem,
    g_ssem,
    g_rsem,
    l_ssem,
    l_rsem,
    r_ssem,
    r_rsem,
    n_ssem,
    n_rsem,
    ux_ssem,
    ux_rsem,
    uz_ssem,
    uu_rsem,
    ud_rsem,
):
    f32, bf16 = jnp.float32, jnp.bfloat16
    Z, Q, U = groups, PARTS, PIECES
    own = Z - 1
    width = g.shape[0]
    half = width // 2
    rows = half // Q
    cols = d.shape[2]
    span = first.shape[0]
    replica, s = lax.axis_index("replica"), lax.axis_index("shard")
    z, x = lax.div(replica, 2), lax.rem(replica, 2)
    y, c = lax.div(s, 2), lax.rem(s, 2)
    i = x * 4 + s
    x_dev = (z * 2 + 1 - x, s)
    y_dev = (replica, (1 - y) * 2 + c)
    c_dev = (replica, y * 2 + 1 - c)
    up_dev = (replica + 2, s)
    down_dev = (replica - 2, s)

    def remote(src, dst, ssem, rsem, dev):
        return pltpu.make_async_remote_copy(
            src_ref=src,
            dst_ref=dst,
            send_sem=ssem,
            recv_sem=rsem,
            device_id=dev,
            device_id_type=pl.DeviceIdType.MESH,
        )

    def peer(k):
        j = lax.rem(i + k, 8)
        return (z * 2 + lax.div(j, 4), lax.rem(j, 4))

    loads = [
        pltpu.make_async_copy(roots_hbm, roots, load_sem.at[0]),
        pltpu.make_async_copy(first_hbm, first, load_sem.at[1]),
        pltpu.make_async_copy(second_hbm, second, load_sem.at[2]),
        pltpu.make_async_copy(stats_hbm, stats, load_sem.at[3]),
    ]

    barrier = pltpu.get_barrier_semaphore()

    def greet(dev):
        pl.semaphore_signal(barrier, inc=1, device_id=dev, device_id_type=pl.DeviceIdType.MESH)

    for k in range(1, 8):
        greet(peer(k))
    has_below, has_above = z > 0, z < Z - 1

    @pl.when(has_above)
    def _():
        greet(up_dev)

    @pl.when(has_below)
    def _():
        greet(down_dev)

    for load in loads:
        load.start()
    orders = block_orders(Z)

    def target(k):
        return sum(
            is_equal(z, p) * is_equal(k, q) * orders[p][q] for p in range(Z) for q in range(Z)
        )

    def x_copy(k, q):
        return remote(x_send.at[k, q], x_recv.at[k, q], x_ssem.at[k, q], x_rsem.at[k, q], x_dev)

    def up_copy(k, m, t):
        return remote(z_send.at[k, m], up_recv.at[t, m], z_ssem.at[k, m], up_rsem.at[t, m], up_dev)

    def down_copy(k, m, t):
        return remote(
            z_send.at[k, m], down_recv.at[t, m], z_ssem.at[k, m], down_rsem.at[t, m], down_dev
        )

    def awaited(t):
        return (t > z) & has_below, (t < z) & has_above

    def gather(ref, k, m, t, from_below, from_above):
        @pl.when(from_below)
        def _():
            up_copy(k, m, t).wait_recv()
            ref[...] = ref[...] + up_recv[t, m].astype(f32)

        @pl.when(from_above)
        def _():
            down_copy(k, m, t).wait_recv()
            ref[...] = ref[...] + down_recv[t, m].astype(f32)

    def pass_on(ref, k, m):
        t = target(k)
        gather(ref, k, m, t, *awaited(t))
        z_send[k, m] = ref[...].astype(bf16)

        @pl.when(t > z)
        def _():
            up_copy(k, m, t).start()

        @pl.when(t < z)
        def _():
            down_copy(k, m, t).start()

    def left_rows(shard):
        return left.at[pl.ds(pl.multiple_of(shard * span, span), span)]

    place = right.at[pl.ds(pl.multiple_of(c * span, span), span)]
    at_home = is_equal(x, y) * is_equal(y, c)
    s_y = (1 - y) * 2 + c
    l_y = remote(left_rows(s), left_rows(s), l_ssem.at[0], l_rsem.at[0], y_dev)
    l_c = remote(left_rows(s), left_rows(s), l_ssem.at[1], l_rsem.at[1], c_dev)
    l_f = remote(left_rows(s_y), left_rows(s_y), l_ssem.at[2], l_rsem.at[2], c_dev)

    def r_copy(tx):
        return remote(stage, place, r_ssem.at[tx], r_rsem.at[c], (z * 2 + tx, x * 2 + y))

    def send_roots():
        loads[0].wait()
        stage[...] = roots[:, 1, :]
        for tx in range(2):

            @pl.when(is_equal(x, tx) * at_home == 0)
            def _(tx=tx):
                r_copy(tx).start()

        left_rows(s)[...] = roots[:, 0, :]
        l_y.start()
        l_c.start()

        @pl.when(at_home == 1)
        def _():
            place[...] = stage[...]

    def block_of(t):
        block = jnp.int32(0)
        for b in range(Z):
            block = jnp.where(owner_ref[b] == t, jnp.int32(b), block)
        return block

    def product(k, side, q):
        r = pl.ds(pl.multiple_of(side * half + q * rows, rows), rows)

        @pl.when(k == 0)
        def _():
            at[r, :] = a[:, r].T

        return jnp.dot(at[r, :], d[block_of(target(k))], preferred_element_type=f32)

    def multiply(k, carry):
        t = target(k)

        def send_away(q, carry):
            x_send[k, q - 1] = product(k, 1 - x, q).astype(bf16)

            @pl.when(k < own - 1)
            def _():
                x_copy(k, q - 1).start()

            return carry

        def keep(q, carry):
            acc[k, q] = product(k, x, q)
            return carry

        from_below, from_above = awaited(t)
        waits = from_below | from_above

        def pass_first():
            pass_on(acc.at[k, 0], k, 0)
            pass_on(away0.at[k], k, Q)

        @pl.when(k > 0)
        def _():
            send_away(1, 0)
            keep(0, 0)

        away0[k] = product(k, 1 - x, 0)

        @pl.when((k < own) & jnp.logical_not(waits))
        def _():
            pass_first()

        lax.fori_loop(2, Q, send_away, 0)
        lax.fori_loop(1, Q, keep, 0)

        @pl.when(k == 0)
        def _():
            send_roots()

        @pl.when((k < own) & waits)
        def _():
            pass_first()

        return carry

    x_send[0, 0] = product(jnp.int32(0), 1 - x, 1).astype(bf16)
    acc[0, 0] = product(jnp.int32(0), x, 0)
    pl.semaphore_wait(barrier, 9 - is_equal(z, 0) - is_equal(z, Z - 1))
    x_copy(0, 0).start()
    lax.fori_loop(0, Z, multiply, 0)

    def pass_reduced(n, carry):
        k, q = lax.div(n, Q - 1), lax.rem(n, Q - 1)
        x_copy(k, q).wait_recv()
        acc[k, q + 1] = acc[k, q + 1] + x_recv[k, q].astype(f32)
        pass_on(acc.at[k, q + 1], k, q + 1)
        return carry

    def p_copy(m):
        return remote(p_send.at[m], p_recv.at[m], p_ssem.at[m], p_rsem.at[m], x_dev)

    def own_sum(m):
        ref = away0.at[own] if m == Q else acc.at[own, m]
        gather(ref, own, m, z, has_below, has_above)
        p_send[m] = ref[...].astype(bf16)
        p_copy(m).start()

    def own_first():
        own_sum(0)
        own_sum(Q)
        for k in (own - 1, own):
            for q in range(Q - 1):
                x_copy(k, q).start()

    @pl.when(has_below & has_above)
    def _():
        own_first()

    lax.fori_loop(0, (own - 1) * (Q - 1), pass_reduced, 0)
    l_y.wait_recv()
    l_f.start()

    @pl.when(jnp.logical_not(has_below & has_above))
    def _():
        own_first()

    def tile(cc, shard):
        top = pl.multiple_of(cc * rows, rows)
        side = pl.multiple_of(shard * cols, cols)
        return g.at[pl.ds(top, rows), pl.ds(side, cols)]

    def g_copy(rel, cc):
        ref = tile(cc, s_y if rel == 2 else s)
        dev = y_dev if rel == 1 else c_dev
        return remote(ref, ref, g_ssem.at[rel, cc], g_rsem.at[rel, cc], dev)

    plan = [(0, 0), (1, 0)] + [(0, q) for q in range(1, Q)] + [(1, q) for q in range(1, Q)]

    last = len(plan)

    def chunk(j):
        side, q = plan[j]
        return (x if side == 0 else 1 - x) * Q + q

    def put(j):
        side, q = plan[j]
        if side == 0 and q > 0:
            own_sum(q)
            x_copy(own, q - 1).wait_recv()
            value = acc[own, q] + x_recv[own, q - 1].astype(f32)
        elif side == 0:
            p_copy(Q).wait_recv()
            value = acc[own, 0] + p_recv[Q].astype(f32)
        elif q == 0:
            p_copy(0).wait_recv()
            value = away0[own] + p_recv[0].astype(f32)
        else:
            p_copy(q).wait_recv()
            value = x_send[own, q - 1].astype(f32) + p_recv[q].astype(f32)
        cc = chunk(j)
        tile(cc, s)[...] = value.astype(bf16)
        g_copy(1, cc).start()
        g_copy(0, cc).start()

    def forward(j):
        g_copy(1, chunk(j)).wait_recv()
        g_copy(2, chunk(j)).start()

    def precondition(j):
        cc = chunk(j)
        g_copy(0, cc).wait_recv()
        g_copy(2, cc).wait_recv()
        r = pl.ds(pl.multiple_of(cc * rows, rows), rows)
        value = lax.dot_general(
            g[r, :], right[...], (((1,), (1,)), ((), ())), preferred_element_type=f32
        )
        top = value.astype(bf16)
        high[...] = top
        low[...] = (value - top.astype(f32)).astype(bf16)

        def times_left(n, total):
            o = pl.ds(pl.multiple_of(n * rows, rows), rows)
            value = jnp.dot(left[o, r], high[...], preferred_element_type=f32) + jnp.dot(
                left[o, r], low[...], preferred_element_type=f32
            )
            value = value if j == 0 else precond[o, :] + value
            precond[o, :] = value
            return total + value * value if j == last - 1 else total

        return lax.fori_loop(0, Q, times_left, jnp.zeros((rows, cols), f32) if j == last - 1 else 0)

    base = pl.multiple_of(i * span, span)
    lot = 16

    def adam(n, carry):
        total, first_bias, second_bias = carry
        r = pl.ds(pl.multiple_of(n * lot, lot), lot)
        grad = g[pl.ds(pl.multiple_of(base + n * lot, lot), lot), :].astype(f32)
        first_new = beta_first * first[r, :] + (1.0 - beta_first) * grad
        second_new = beta_second * second[r, :] + (1.0 - beta_second) * grad * grad
        first[r, :] = first_new
        second[r, :] = second_new
        value = (first_new * first_bias) / (jnp.sqrt(second_new * second_bias) + eps_adam)
        return total + value * value, first_bias, second_bias

    def roots_here():
        for rc in range(2):

            @pl.when(at_home * is_equal(c, rc) == 0)
            def _(rc=rc):
                remote(
                    stage, right.at[pl.ds(rc * span, span)], r_ssem.at[0], r_rsem.at[rc], x_dev
                ).wait_recv()

        l_c.wait_recv()
        l_f.wait_recv()

    def adam_sum():
        for load in loads[1:]:
            load.wait()
        first_bias = 1.0 / jnp.full((1, width), 1.0 - power(beta_first, count_ref[0]))
        second_bias = 1.0 / jnp.full((1, width), 1.0 - power(beta_second, count_ref[0]))
        total, _, _ = lax.fori_loop(
            0, span // lot, adam, (jnp.zeros((lot, width), f32), first_bias, second_bias)
        )
        return jnp.sum(total)

    for j in range(last):
        if j == 2:
            lax.fori_loop((own - 1) * (Q - 1), own * (Q - 1), pass_reduced, 0)
        put(j)
        if j >= 2:
            forward(j - 2)
        if j == 3:
            roots_here()
        if j >= 3:
            precondition(j - 3)
    forward(last - 2)
    precondition(last - 3)
    precondition(last - 2)
    forward(last - 1)
    adam_squares = adam_sum()
    precond_squares = jnp.sum(precondition(last - 1))

    which = lax.broadcasted_iota(jnp.int32, norms.shape[1:], 0)
    norms[i] = jnp.where(which == 0, adam_squares, precond_squares)

    def n_copy(k):
        return remote(norms.at[i], norms.at[i], n_ssem.at[k - 1], n_rsem.at[i], peer(k))

    for k in range(1, 8):
        n_copy(k).start()
    for k in range(1, 8):
        j = lax.rem(i + k, 8)
        remote(norms.at[j], norms.at[j], n_ssem.at[k - 1], n_rsem.at[j], peer(k)).wait_recv()
    total = norms[0]
    for k in range(1, 8):
        total = total + norms[k]
    scale = jnp.sqrt(total[0:1, :]) / (jnp.sqrt(total[1:2, :]) + eps_norm)
    scale = jnp.concatenate([scale] * (cols // 128), axis=1)

    piece = half // U

    def part(zt, xt, q):
        top = pl.multiple_of(xt * half + q * piece, piece)
        return u.at[zt, pl.ds(top, piece), :]

    def z_part(zt, m):
        return part(zt, 1 - x, 0) if m == U else part(zt, x, m)

    def ux_copy(zt, q):
        return remote(part(zt, x, q), part(zt, x, q), ux_ssem.at[zt, q], ux_rsem.at[zt, q], x_dev)

    def uu_copy(zt, m):
        return remote(z_part(zt, m), z_part(zt, m), uz_ssem.at[0, zt, m], uu_rsem.at[zt, m], up_dev)

    def ud_copy(zt, m):
        return remote(z_part(zt, m), z_part(zt, m), uz_ssem.at[1, zt, m], ud_rsem.at[zt, m], down_dev)

    def spread(m):
        @pl.when(has_above)
        def _():
            uu_copy(z, m).start()

        @pl.when(has_below)
        def _():
            ud_copy(z, m).start()

    for q in range(U):
        part(z, x, q)[...] = (precond[pl.ds(q * piece, piece), :] * scale).astype(bf16)
        ux_copy(z, q).start()
        spread(q)
    ux_copy(z, 0).wait_recv()
    spread(U)

    window = pl.multiple_of(lax.div(i, 2) * cols, cols)
    turned = g[:, pl.ds(window, cols)].T
    columns[...] = jnp.where(lax.rem(i, 2) == 1, turned[span:, :], turned[:span, :])

    def grams(n, carry):
        r = pl.ds(pl.multiple_of(n * cols, cols), cols)
        left_gram = lax.dot_general(
            g[pl.ds(base, span), :], g[r, :], (((1,), (1,)), ((), ())), preferred_element_type=f32
        )
        stats[:, 0, r] = beta_stat * stats[:, 0, r] + (1.0 - beta_stat) * left_gram
        right_gram = jnp.dot(columns[...], g[:, r], preferred_element_type=f32)
        stats[:, 1, r] = beta_stat * stats[:, 1, r] + (1.0 - beta_stat) * right_gram
        return carry

    lax.fori_loop(0, width // cols, grams, 0)

    def relay(zt, m, copy, onward):
        copy(zt, m).wait_recv()

        @pl.when(onward)
        def _():
            copy(zt, m).start()

        if 0 < m < U:
            ux_copy(zt, m).start()

    for dist in range(1, Z):

        @pl.when(z - dist >= 0)
        def _(dist=dist):
            relay(z - dist, 0, uu_copy, has_above)

        @pl.when(z + dist < Z)
        def _(dist=dist):
            relay(z + dist, 0, ud_copy, has_below)

        for m in range(1, U + 1):

            @pl.when(z - dist >= 0)
            def _(dist=dist, m=m):
                relay(z - dist, m, uu_copy, has_above)

            @pl.when(z + dist < Z)
            def _(dist=dist, m=m):
                relay(z + dist, m, ud_copy, has_below)

    def arrive(zt):
        for q in range(1, U):
            ux_copy(zt, q).wait_recv()

    arrive(z)
    for dist in range(1, Z):

        @pl.when(z - dist >= 0)
        def _(dist=dist):
            arrive(z - dist)

        @pl.when(z + dist < Z)
        def _(dist=dist):
            arrive(z + dist)

    l_y.wait_send()
    l_c.wait_send()
    l_f.wait_send()
    for tx in range(2):

        @pl.when(is_equal(x, tx) * at_home == 0)
        def _(tx=tx):
            r_copy(tx).wait_send()

    for k in range(1, 8):
        n_copy(k).wait_send()

    def sent(k, carry):
        for q in range(Q - 1):
            x_copy(k, q).wait_send()

        @pl.when(k < Z - 1)
        def _():
            for m in range(Q + 1):
                up_copy(k, m, k).wait_send()

        ux_last = is_equal(k, z)

        @pl.when(ux_last == 1)
        def _():
            ux_copy(k, 0).wait_send()

        for q in range(1, U):
            ux_copy(k, q).wait_send()

        @pl.when((z >= k) & has_above)
        def _():
            for m in range(U + 1):
                uu_copy(k, m).wait_send()

        @pl.when((z <= k) & has_below)
        def _():
            for m in range(U + 1):
                ud_copy(k, m).wait_send()

        return carry

    lax.fori_loop(0, Z, sent, 0)
    for m in range(Q + 1):
        p_copy(m).wait_send()
    for rel in range(3):
        for cc in range(2 * Q):
            g_copy(rel, cc).wait_send()


def finish_kernel(owner_ref, u, first, second, stats, update, first_out, second_out, stats_out, sems):
    copies = [
        pltpu.make_async_copy(u.at[owner_ref[b]], update.at[b], sems.at[b])
        for b in range(u.shape[0])
    ]
    for ref, out in ((stats, stats_out), (first, first_out), (second, second_out)):
        copies.append(pltpu.make_async_copy(ref, out, sems.at[len(copies)]))
    for copy in copies:
        copy.start()
    for copy in copies:
        copy.wait()


def fused_body(
    activations,
    output_grads,
    owner,
    step_count,
    statistics,
    inverse_roots,
    first_moment,
    second_moment,
):
    f32, bf16 = jnp.float32, jnp.bfloat16
    tokens, width = activations.shape
    groups, cols = output_grads.shape[1:]
    span = statistics.shape[0]
    half, Q, U = width // 2, PARTS, PIECES
    rows = half // Q

    VMEM, DMA = pltpu.VMEM, pltpu.SemaphoreType.DMA
    hbm = pl.BlockSpec(memory_space=pl.ANY)
    smem = pl.BlockSpec(memory_space=pltpu.SMEM)
    results = (
        jax.ShapeDtypeStruct((groups, width, cols), bf16),
        jax.ShapeDtypeStruct((span, width), f32),
        jax.ShapeDtypeStruct((span, width), f32),
        jax.ShapeDtypeStruct((span, 2, width), f32),
    )
    vmem = pl.BlockSpec(memory_space=pltpu.VMEM)
    update, first_new, second_new, new_stats = pl.pallas_call(
        functools.partial(step_kernel, groups),
        out_shape=tuple(VMEM(r.shape, r.dtype) for r in results),
        in_specs=[smem, smem, vmem, vmem] + [hbm] * 4,
        out_specs=[vmem] * 4,
        scratch_shapes=[
            VMEM((width, tokens), bf16),
            VMEM((groups, Q, rows, cols), f32),
            VMEM((groups, rows, cols), f32),
            VMEM((groups, Q - 1, rows, cols), bf16),
            VMEM((groups, Q - 1, rows, cols), bf16),
            VMEM((groups, Q + 1, rows, cols), bf16),
            VMEM((groups, Q + 1, rows, cols), bf16),
            VMEM((groups, Q + 1, rows, cols), bf16),
            VMEM((Q + 1, rows, cols), bf16),
            VMEM((Q + 1, rows, cols), bf16),
            VMEM((width, width), bf16),
            VMEM((half, width), bf16),
            VMEM((2 * span, width), bf16),
            VMEM((span, width), bf16),
            VMEM((span, 2, width), bf16),
            VMEM((rows, cols), bf16),
            VMEM((rows, cols), bf16),
            VMEM((half, cols), f32),
            VMEM((span, width), bf16),
            VMEM((8, 8, 128), f32),
            DMA((4,)),
            DMA((groups, Q - 1)),
            DMA((groups, Q - 1)),
            DMA((Q + 1,)),
            DMA((Q + 1,)),
            DMA((groups, Q + 1)),
            DMA((groups, Q + 1)),
            DMA((groups, Q + 1)),
            DMA((3, 2 * Q)),
            DMA((3, 2 * Q)),
            DMA((3,)),
            DMA((3,)),
            DMA((2,)),
            DMA((2,)),
            DMA((7,)),
            DMA((8,)),
            DMA((groups, U)),
            DMA((groups, U)),
            DMA((2, groups, U + 1)),
            DMA((groups, U + 1)),
            DMA((groups, U + 1)),
        ],
        compiler_params=pltpu.CompilerParams(
            collective_id=0, has_side_effects=True, vmem_limit_bytes=44 * 1024 * 1024
        ),
        name="step_kernel",
    )(
        owner,
        step_count,
        pltpu.with_memory_space_constraint(activations, pltpu.VMEM),
        pltpu.with_memory_space_constraint(output_grads.transpose(1, 0, 2), pltpu.VMEM),
        inverse_roots,
        first_moment,
        second_moment,
        statistics,
    )
    update, first_new, second_new, new_stats = pl.pallas_call(
        finish_kernel,
        out_shape=results,
        in_specs=[smem] + [vmem] * 4,
        out_specs=[hbm] * 4,
        scratch_shapes=[DMA((groups + 3,))],
        compiler_params=pltpu.CompilerParams(vmem_limit_bytes=16 * 1024 * 1024),
        name="finish_kernel",
    )(owner, update, first_new, second_new, new_stats)
    return (new_stats, first_new, second_new, update)


def dispatch(replicas, shards, *args):
    width, groups, cols = args[0].shape[1], args[1].shape[1], args[1].shape[2]
    whole = width % (256 * PARTS) == 0 and width % (256 * PIECES) == 0 and cols % 128 == 0
    if replicas == 2 * groups and shards == 4 and whole:
        return fused_body(*args)
    return body(*args)


def solution(mesh):
    placed = (
        P("replica", None),
        P("replica", None, "shard"),
        P(),
        P(),
        P(("replica", "shard"), None, None),
        P(("replica", "shard"), None, None),
        P(("replica", "shard"), None),
        P(("replica", "shard"), None),
    )
    return jax.shard_map(
        functools.partial(dispatch, mesh.shape["replica"], mesh.shape["shard"]),
        mesh=mesh,
        in_specs=placed,
        out_specs=(
            P(("replica", "shard"), None, None),
            P(("replica", "shard"), None),
            P(("replica", "shard"), None),
            P(None, None, "shard"),
        ),
        check_vma=False,
    )
```
